256 devices in a mesh: aux: 64 (over x, z, core), pair: 4 (over y).
Axes of the slice: x: 4, y: 4, z: 8, core: 2. Of those that a mesh axis runs over, the one named last changes fastest.
Arguments:
- three_centre: bfloat16 [16, 1280, 128, 128], P('pair', 'aux'), may hold values from -6 to 6
- block_mask: int32 [16], replicated, may hold values from 0 to 1, as said below
- block_owner: int32 [16], replicated, may hold values from 0 to 3, as said below
- block_index: int32 [2, 16], replicated, may hold values from 0 to 23
- active_orbitals: bfloat16 [24, 3072], replicated, may hold values from -0.5 to 0.5
- inactive_orbitals: bfloat16 [256, 3072], replicated, may hold values from -0.75 to 0.75
Outputs:
- fock_blocks: float32 [32, 128, 128], P('pair')
- active_integrals: float32 [576, 576], P('aux')
The draws below stay inside these ranges and needn't reach their ends.
Inputs may be any that keep to these rules, and one draw needn't show every extreme that they name: `block_mask`: every index of pair holds at least 2 live slots. `block_owner`: among the 4 slots of one index of pair, live or not, at most 2 name any one owner; one owner is named by exactly 2 live slots of every index of pair, so it receives 8 live blocks.
All inputs are finite; a program needn't handle non-finite values.
Results may differ from the reference program's by a relative error of at most 0.0044.
Values may be sent and summed in bfloat16 or wider, within the bound.
No kernel may reach another device: no remote copies, remote signals or barrier semaphores. Data moves between devices by JAX's collectives and lax.ppermute only.
A program may use at most 64 MiB of HBM per device.

```python
import math
import jax
import jax.numpy as jnp
from jax import lax

NAO = 3072
BW = 128
NB = 24
ACT = 24
PAIRS = 576
NIN = 256
AUX = 1280
SLOT_IN = 4
SLOTS = 16
OWN = 8
N_PAIR = 4


def owner_plan(key):
    capacity = SLOT_IN // 2
    hottest = jax.random.randint(jax.random.fold_in(key, 11), (), 0, N_PAIR)
    owner_parts = []
    mask_parts = []
    for source in range(N_PAIR):
        source_key = jax.random.fold_in(key, 100 + source)
        ticket_key, live_key, order_key = jax.random.split(source_key, 3)
        tickets = jax.random.permutation(ticket_key, (N_PAIR - 1) * capacity)[:SLOT_IN - capacity] // capacity
        others = (hottest + 1 + tickets) % N_PAIR
        sequence = jnp.concatenate([jnp.full((capacity,), hottest, jnp.int32), others.astype(jnp.int32)])
        living = jnp.concatenate([jnp.ones((capacity,), jnp.int32), jax.random.randint(live_key, (SLOT_IN - capacity,), 0, 2).astype(jnp.int32)])
        ordering = jax.random.permutation(order_key, SLOT_IN)
        owner_parts.append(sequence[ordering])
        mask_parts.append(living[ordering])
    return (jnp.concatenate(owner_parts).astype(jnp.int32), jnp.concatenate(mask_parts).astype(jnp.int32))


def draw_block_mask(key, part):
    return owner_plan(jax.random.fold_in(key, 7))[1]


def draw_block_owner(key, part):
    return owner_plan(jax.random.fold_in(key, 7))[0]


def touch_ends(array, own_key, least, top_value):
    longest = array.shape.index(max(array.shape))
    spots = []
    for shift in (0, 1):
        where = [jax.random.randint(jax.random.fold_in(own_key, axis), (), 0, length) for axis, length in enumerate(array.shape)]
        where[longest] = (where[longest] + shift) % array.shape[longest]
        spots.append(tuple(where))
    return array.at[spots[0]].set(least).at[spots[1]].set(top_value)


def block_scale(stream_key, extent, cuts, low, top_value):
    def one(axis_at, parts):
        steps = jax.random.uniform(jax.random.fold_in(jax.random.fold_in(stream_key, 6), axis_at), (parts,), jnp.float32, low / len(cuts), top_value / len(cuts))
        return jnp.repeat(jnp.exp(steps), extent[axis_at] // parts).reshape((-1,) + (1,) * (len(extent) - axis_at - 1))

    loudness = one(*cuts[0])
    for cut in cuts[1:]:
        loudness = loudness * one(*cut)
    return loudness


def centred(key, shape, deviation, reach, shards=(), held_as=jnp.bfloat16):
    result = jax.random.normal(key, shape, jnp.float32) * deviation
    if len(shards) > 0:
        result = block_scale(key, shape, shards, -0.22, 0.18) * result
    return jnp.clip(result, min=-reach, max=reach).astype(held_as)


def setup_inputs(seed: int = 0) -> dict:
    arg_keys = jax.random.split(jax.random.key(seed), 7)
    three_centre = centred(arg_keys[0], (SLOTS, AUX, BW, BW), 1.0, 6.0, ((0, 4), (1, 64)))
    block_mask = draw_block_mask(jax.random.fold_in(arg_keys[6], 71), 0)
    block_owner = draw_block_owner(jax.random.fold_in(arg_keys[6], 71), 0)
    block_index = touch_ends(jax.random.randint(arg_keys[3], (2, SLOTS), 0, NB), jax.random.fold_in(arg_keys[3], 1), 0, NB - 1).astype(jnp.int32)
    active_orbitals = centred(arg_keys[4], (ACT, NAO), BW ** -0.5, 0.5)
    inactive_orbitals = centred(arg_keys[5], (NIN, NAO), (NIN // 4) ** -0.5, 0.75)
    return dict(three_centre=three_centre, block_mask=block_mask, block_owner=block_owner, block_index=block_index, active_orbitals=active_orbitals, inactive_orbitals=inactive_orbitals)


def one_slot(block, row_block, col_block, living, active_split, inactive_split):
    active_rows = active_split[:, row_block, :].astype(jnp.float32)
    active_cols = active_split[:, col_block, :].astype(jnp.float32)
    half_done = jnp.einsum('pab,ub->pua', block.astype(jnp.float32), active_cols).astype(jnp.bfloat16)
    fitted = jnp.einsum('pua,ta->ptu', half_done.astype(jnp.float32), active_rows) * living
    inactive_rows = inactive_split[:, row_block, :].astype(jnp.float32)
    inactive_cols = inactive_split[:, col_block, :].astype(jnp.float32)
    density = jnp.einsum('ka,kb->ab', inactive_rows, inactive_cols).astype(jnp.bfloat16)
    coupling = jnp.einsum('pab,ab->p', block.astype(jnp.float32), density.astype(jnp.float32)) * living / BW
    return (fitted.reshape(AUX, PAIRS), coupling)

def reference(three_centre, block_mask, block_owner, block_index, active_orbitals, inactive_orbitals):
    active_split = active_orbitals.reshape(ACT, NB, BW)
    inactive_split = inactive_orbitals.reshape(NIN, NB, BW)
    living_all = block_mask.astype(jnp.float32)

    def fitted_step(carry, inputs):
        block, row_block, col_block, living = inputs
        fitted, coupling = one_slot(block, row_block, col_block, living, active_split, inactive_split)
        return ((carry[0] + fitted, carry[1] + coupling), None)
    start_values = (jnp.zeros((AUX, PAIRS), jnp.float32), jnp.zeros((AUX,), jnp.float32))
    (fitted_sum, coupling_sum), _ = lax.scan(fitted_step, start_values, (three_centre, block_index[0], block_index[1], living_all))
    fitted = fitted_sum.astype(jnp.bfloat16)
    coupling = coupling_sum.astype(jnp.bfloat16).astype(jnp.float32)

    def coulomb_of(block):
        return jnp.einsum('pab,p->ab', block.astype(jnp.float32), coupling) / math.sqrt(AUX)
    coulomb = lax.map(coulomb_of, three_centre)
    owners = jnp.arange(N_PAIR, dtype=jnp.int32)
    flagged = ((block_owner[:, None] == owners[None, :]) & (block_mask[:, None] == 1)).astype(jnp.int32)
    slot_rank = lax.optimization_barrier(jnp.sum((jnp.cumsum(flagged, axis=0) - flagged) * flagged, axis=1))
    ranks = jnp.arange(OWN, dtype=jnp.int32)
    selector = flagged.T[:, None, :].astype(jnp.float32) * (slot_rank[None, None, :] == ranks[None, :, None]).astype(jnp.float32)
    fock_blocks = jnp.einsum('okg,gab->okab', selector, coulomb, precision=lax.Precision.HIGHEST).reshape(N_PAIR * OWN, BW, BW)
    active_integrals = jnp.dot(fitted.T, fitted, preferred_element_type=jnp.float32) / AUX
    return (fock_blocks, active_integrals)
```

```python
import math

import jax
import jax.numpy as jnp
from jax import lax
from jax.experimental import pallas as pl
from jax.experimental.pallas import tpu as pltpu
from jax.sharding import Mesh, PartitionSpec as P

SLOTS = 4
ROWS = 20
BW = 128
ACT = 24
PAIRS = 576
GROUPS = 4
PER = 5
USED = PER * ACT
CHIPS = 32
CORES = 2
OWNERS = 4
AUX = 1280
MSG = 24
F32 = jnp.float32
BF16 = jnp.bfloat16

ANY = pl.BlockSpec(memory_space=pl.ANY)
VMEM = pl.BlockSpec(memory_space=pltpu.VMEM)
SMEM = pl.BlockSpec(memory_space=pltpu.SMEM)


def nt(a, b):
    return lax.dot_general(a, b, (((1,), (1,)), ((), ())), preferred_element_type=F32)


def lanes(shape):
    return lax.broadcasted_iota(jnp.int32, shape, len(shape) - 1)


def sublanes(shape):
    return lax.broadcasted_iota(jnp.int32, shape, len(shape) - 2)


def contract_kernel(
    mask_ref, index_ref, blocks_hbm, active_hbm, inactive_hbm, out_ref,
    blocks, act_row, act_col, ina_row, ina_col, wide, halves, sums,
    block_sem, ar_sem, ac_sem, ir_sem, ic_sem,
):
    here = lax.axis_index("pair")
    copies = []
    for g in range(SLOTS):
        slot = here * SLOTS + g
        row = pl.multiple_of(index_ref[0, slot] * BW, BW)
        col = pl.multiple_of(index_ref[1, slot] * BW, BW)
        group = [
            pltpu.make_async_copy(inactive_hbm.at[:, pl.ds(row, BW)], ina_row.at[g], ir_sem.at[g]),
            pltpu.make_async_copy(inactive_hbm.at[:, pl.ds(col, BW)], ina_col.at[g], ic_sem.at[g]),
            pltpu.make_async_copy(active_hbm.at[:, pl.ds(row, BW)], act_row.at[g], ar_sem.at[g]),
            pltpu.make_async_copy(active_hbm.at[:, pl.ds(col, BW)], act_col.at[g], ac_sem.at[g]),
            pltpu.make_async_copy(blocks_hbm.at[g], blocks.at[g], block_sem.at[g]),
        ]
        for c in group:
            c.start()
        copies.append(group)
    wide[...] = jnp.zeros_like(wide)
    for g in range(SLOTS):
        live = mask_ref[here * SLOTS + g].astype(F32)
        for c in copies[g]:
            c.wait()
        density = lax.dot_general(
            ina_row[g], ina_col[g], (((0,), (0,)), ((), ())), preferred_element_type=F32
        )
        density = density.astype(BF16).astype(F32) * live
        for p in range(ROWS):
            product = blocks[g, p].astype(F32) * density
            part = jnp.sum(product.reshape(BW // 8, 8, BW), axis=0)
            if g == 0:
                sums[p] = part
            else:
                sums[p] = sums[p] + part
        column = act_col[g].astype(F32)
        for p in range(PER):
            wide[pl.ds(ACT * p, ACT), pl.ds(BW * p, BW)] = column
        weights = wide[...].astype(BF16)
        for k in range(GROUPS):
            joined = jnp.concatenate([blocks[g, k * PER + p] for p in range(PER)], axis=1)
            half = nt(joined, weights)
            halves[pl.ds(g * BW, BW), pl.ds(k * BW, BW)] = half.astype(BF16)
    rows = jnp.concatenate(
        [
            act_row[g].astype(F32) * mask_ref[here * SLOTS + g].astype(F32)
            for g in range(SLOTS)
        ],
        axis=1,
    ).astype(BF16)
    fitted = jnp.dot(rows, halves[...], preferred_element_type=F32)
    coupling = jnp.sum(jnp.sum(sums[...], axis=1), axis=1, keepdims=True) * (1.0 / BW)
    coupling = jnp.concatenate([coupling, jnp.zeros((ACT - ROWS, 1), F32)], axis=0)
    high = coupling.astype(BF16).astype(F32)
    low = coupling - high
    spare = lanes((ACT, BW)) >= USED
    for k in range(GROUPS):
        tail = high if k == 0 else low if k == 1 else jnp.zeros_like(high)
        tile = jnp.where(spare, jnp.broadcast_to(tail, (ACT, BW)), fitted[:, k * BW : (k + 1) * BW])
        out_ref[:, pl.ds(k * BW, BW)] = tile.astype(BF16)


def expand_kernel(
    own_ref, one_ref, two_ref, three_ref, blocks_hbm, keep_ref, send_ref,
    blocks, coupling_ref, spread, left, coulomb, main, rest, block_sem,
):
    here = lax.axis_index("pair")
    core = lax.axis_index("core")
    copies = [
        pltpu.make_async_copy(blocks_hbm.at[g], blocks.at[g], block_sem.at[g]) for g in range(SLOTS)
    ]
    for c in copies:
        c.start()
    total = (own_ref[...].astype(F32) + two_ref[...].astype(F32)) + (
        one_ref[...].astype(F32) + three_ref[...].astype(F32)
    )
    both = total[:, :BW] + total[:, BW : 2 * BW]
    coupling = jnp.sum(jnp.where(lanes((ACT, BW)) == USED, both, 0.0), axis=1, keepdims=True)
    coupling_ref[...] = jnp.broadcast_to(coupling.astype(BF16).astype(F32), (ACT, BW))
    fitted = total.astype(BF16).astype(F32)
    offset = lanes((ACT, BW)) - sublanes((ACT, BW))
    keep = offset == 0
    for p in range(1, PER):
        keep = keep | (offset == ACT * p)
    keep = jnp.concatenate([keep.astype(F32)] * GROUPS, axis=1)
    for t in range(0, ACT, 2):
        pair = jnp.concatenate(
            [jnp.broadcast_to(fitted[t + d : t + d + 1, :], keep.shape) * keep for d in range(2)],
            axis=0,
        )
        spread[pl.ds(t * ACT, 2 * ACT), :] = pair.astype(BF16)
    shape = (GROUPS * BW, BW)
    lane = lanes(shape)
    group = (
        (lane >= PER).astype(jnp.int32)
        + (lane >= 2 * PER).astype(jnp.int32)
        + (lane >= 3 * PER).astype(jnp.int32)
    )
    start = group * BW + (lane - group * PER) * ACT
    position = sublanes(shape) - start
    pick = (position >= 0) & (position < ACT) & (lane < ROWS)
    folded = jnp.dot(
        spread[...], pick.astype(F32).astype(BF16), preferred_element_type=F32
    ).astype(BF16)
    left[...] = folded
    columns = left[pl.ds(pl.multiple_of(here * BW, BW), BW), :]
    tail = left[pl.ds(4 * BW, PAIRS - 4 * BW), :]
    main[...] = nt(folded, columns)
    rest[...] = nt(folded, jnp.concatenate([tail, tail], axis=0))
    for g in range(SLOTS):
        copies[g].wait()
        total_g = jnp.zeros((BW, BW), F32)
        for p in range(ROWS):
            factor = jnp.broadcast_to(coupling_ref[pl.ds(p, 1), :], (BW, BW))
            total_g = total_g + blocks[g, p].astype(F32) * factor
        coulomb[pl.ds(g * BW, BW), :] = total_g
    low_lane = lanes((CHIPS, BW)) < BW // 2
    for ref, which in ((keep_ref, core), (send_ref, 1 - core)):
        for g in range(SLOTS):
            for s in range(2):
                value = coulomb[pl.ds(g * BW + s * (BW // 2) + which, CHIPS, stride=2), :]
                ref[pl.ds(2 * g + s, CHIPS, stride=MSG), :] = value
        for s in range(9):
            ref[pl.ds(8 + s, CHIPS, stride=MSG), :] = main[pl.ds(9 * which + s, CHIPS, stride=18), :]
        for s in range(7):
            value = rest[pl.ds(9 * which + s, CHIPS, stride=18), :]
            if s < 2:
                other = rest[pl.ds(9 * which + 7 + s, CHIPS, stride=18), :]
                value = jnp.where(low_lane, value, other)
            ref[pl.ds(17 + s, CHIPS, stride=MSG), :] = value


def route_kernel(mask_ref, owner_ref, parts_ref, out_ref, gram_ref, tile):
    here = lax.axis_index("pair")
    total = jnp.sum(parts_ref[...].astype(F32), axis=0)
    gram_ref[...] = total[8:MSG] * (1.0 / AUX)
    scaled = total[0:8] * (1.0 / math.sqrt(AUX))
    tile[...] = jnp.zeros_like(tile)
    for o in range(OWNERS):
        place = jnp.int32(0)
        for g in range(SLOTS):
            slot = here * SLOTS + g
            chosen = (mask_ref[slot] == 1) & (owner_ref[slot] == o)

            @pl.when(chosen & (place < 2))
            def _(o=o, g=g, place=place):
                tile[o, pl.ds(2 * place, 2), :] = scaled[2 * g : 2 * g + 2]

            place = place + chosen.astype(jnp.int32)
    for o in range(OWNERS):
        piece = tile[o, 0:4, :]
        many = jnp.broadcast_to(piece[None], (CHIPS, 4, BW)).reshape(CHIPS * 4, BW)
        out_ref[pl.ds(o * CHIPS * 4, CHIPS * 4), :] = many.astype(BF16)


def place_kernel(
    mask_ref, owner_ref, own_ref, other_ref, g0_ref, g1_ref, g2_ref, g3_ref,
    fock_ref, gram_ref, wide,
):
    here = lax.axis_index("pair")
    core = lax.axis_index("core")
    fock_ref[...] = jnp.zeros_like(fock_ref)
    wide[0] = own_ref[...].astype(F32)
    wide[1] = other_ref[...].astype(F32)
    rank = jnp.int32(0)
    for q in range(OWNERS):
        place = jnp.int32(0)
        for g in range(SLOTS):
            slot = q * SLOTS + g
            chosen = (mask_ref[slot] == 1) & (owner_ref[slot] == here)

            @pl.when(chosen & (place < 2))
            def _(q=q, rank=rank, place=place):
                for n in range(2):
                    which = core if n == 0 else 1 - core
                    for s in range(2):
                        value = wide[n, pl.ds(q * CHIPS * 4 + 2 * place + s, CHIPS, stride=4), :]
                        fock_ref[pl.ds(rank * BW + s * (BW // 2) + which, CHIPS, stride=2), :] = value

            place = place + chosen.astype(jnp.int32)
            rank = rank + chosen.astype(jnp.int32)
    for n, ref in enumerate((g0_ref, g1_ref, g2_ref, g3_ref)):
        source = lax.rem(here + OWNERS - n, OWNERS)
        gram_ref[:, pl.ds(pl.multiple_of(source * BW, BW), BW)] = ref[0:9, :]
    gram_ref[0:7, pl.ds(4 * BW, BW // 2)] = g0_ref[9:16, 0 : BW // 2]
    gram_ref[7:9, pl.ds(4 * BW, BW // 2)] = g0_ref[9:11, BW // 2 : BW]


def from_others(x):
    return [
        lax.ppermute(x, "pair", [(i, (i + s) % OWNERS) for i in range(OWNERS)])
        for s in range(1, OWNERS)
    ]


def shards(three_centre, block_mask, block_owner, block_index, active_orbitals, inactive_orbitals):
    dma = pltpu.SemaphoreType.DMA
    message = pl.pallas_call(
        contract_kernel,
        out_shape=jax.ShapeDtypeStruct((ACT, GROUPS * BW), BF16),
        in_specs=[SMEM, SMEM, ANY, ANY, ANY],
        out_specs=VMEM,
        scratch_shapes=[
            pltpu.VMEM((SLOTS, ROWS, BW, BW), BF16),
            pltpu.VMEM((SLOTS, ACT, BW), BF16),
            pltpu.VMEM((SLOTS, ACT, BW), BF16),
            pltpu.VMEM((SLOTS, 256, BW), BF16),
            pltpu.VMEM((SLOTS, 256, BW), BF16),
            pltpu.VMEM((BW, PER * BW), F32),
            pltpu.VMEM((SLOTS * BW, GROUPS * BW), BF16),
            pltpu.VMEM((ROWS, 8, BW), F32),
            dma((SLOTS,)), dma((SLOTS,)), dma((SLOTS,)), dma((SLOTS,)), dma((SLOTS,)),
        ],
        name="contract",
    )(block_mask, block_index, three_centre, active_orbitals, inactive_orbitals)
    one, two, three = from_others(message)
    rows = CHIPS * MSG
    keep, send = pl.pallas_call(
        expand_kernel,
        out_shape=[jax.ShapeDtypeStruct((rows, BW), F32)] * 2,
        in_specs=[VMEM, VMEM, VMEM, VMEM, ANY],
        out_specs=[VMEM, VMEM],
        scratch_shapes=[
            pltpu.VMEM((SLOTS, ROWS, BW, BW), BF16),
            pltpu.VMEM((ACT, BW), F32),
            pltpu.VMEM((PAIRS, GROUPS * BW), BF16),
            pltpu.VMEM((PAIRS, BW), BF16),
            pltpu.VMEM((SLOTS * BW, BW), F32),
            pltpu.VMEM((PAIRS, BW), F32),
            pltpu.VMEM((PAIRS, BW), F32),
            dma((SLOTS,)),
        ],
        name="expand",
    )(message, one, two, three, three_centre)
    swap = [(0, 1), (1, 0)]
    chip_sum = (keep + lax.ppermute(send, "core", swap)).astype(BF16)
    parts = lax.all_to_all(chip_sum.reshape(CHIPS, MSG, BW), "chip", 0, 0, tiled=True)
    pieces, gram = pl.pallas_call(
        route_kernel,
        out_shape=[
            jax.ShapeDtypeStruct((OWNERS * CHIPS * 4, BW), BF16),
            jax.ShapeDtypeStruct((16, BW), F32),
        ],
        in_specs=[SMEM, SMEM, VMEM],
        out_specs=[VMEM, VMEM],
        scratch_shapes=[pltpu.VMEM((OWNERS, 8, BW), F32)],
        name="route",
    )(block_mask, block_owner, parts)
    g1, g2, g3 = from_others(gram)
    received = lax.all_to_all(
        pieces.reshape(OWNERS * CHIPS, 4, BW), ("pair", "chip"), 0, 0, tiled=True
    ).reshape(OWNERS * CHIPS * 4, BW)
    partner = lax.ppermute(received, "core", swap)
    fock, integrals = pl.pallas_call(
        place_kernel,
        out_shape=[
            jax.ShapeDtypeStruct((8 * BW, BW), F32),
            jax.ShapeDtypeStruct((9, PAIRS), F32),
        ],
        in_specs=[SMEM, SMEM] + [VMEM] * 6,
        out_specs=[VMEM, VMEM],
        scratch_shapes=[pltpu.VMEM((2, OWNERS * CHIPS * 4, BW), F32)],
        name="place",
    )(block_mask, block_owner, received, partner, gram, g1, g2, g3)
    return (fock.reshape(8, BW, BW), integrals)


def solution(mesh):
    split = Mesh(mesh.devices.reshape(CHIPS, CORES, OWNERS), ("chip", "core", "pair"))
    return jax.shard_map(
        shards,
        mesh=split,
        in_specs=(P("pair", ("chip", "core"), None, None), P(), P(), P(), P(), P()),
        out_specs=(P("pair", None, None), P(("chip", "core"), None)),
        check_vma=False,
    )
```

```python
import math

import jax
import jax.numpy as jnp
from jax import lax
from jax.experimental import pallas as pl
from jax.experimental.pallas import tpu as pltpu
from jax.sharding import Mesh, PartitionSpec as P

SLOTS = 4
ROWS = 20
BW = 128
ACT = 24
PAIRS = 576
GROUPS = 4
PER = 5
USED = PER * ACT
NX = 4
NZ = 8
CHIPS = NX * NZ
CORES = 2
OWNERS = 4
AUX = 1280
MSG = 24
F32 = jnp.float32
BF16 = jnp.bfloat16

HBM = pl.BlockSpec(memory_space=pltpu.HBM)
VMEM = pl.BlockSpec(memory_space=pltpu.VMEM)
SMEM = pl.BlockSpec(memory_space=pltpu.SMEM)


def limit(kib):
    return pltpu.CompilerParams(vmem_limit_bytes=kib << 10)


def nt(a, b):
    return lax.dot_general(a, b, (((1,), (1,)), ((), ())), preferred_element_type=F32)


def lanes(shape):
    return lax.broadcasted_iota(jnp.int32, shape, len(shape) - 1)


def sublanes(shape):
    return lax.broadcasted_iota(jnp.int32, shape, len(shape) - 2)


def contract_kernel(
    mask_hbm, index_hbm, blocks_hbm, active_hbm, inactive_hbm, out_ref, blocks,
    mask_ref, index_ref, act_row, act_col, ina_row, ina_col, wide, halves, sums,
    block_sem, ar_sem, ac_sem, ir_sem, ic_sem, int_sem,
):
    here = lax.axis_index("pair")
    ints = [
        pltpu.make_async_copy(index_hbm, index_ref, int_sem.at[0]),
        pltpu.make_async_copy(mask_hbm, mask_ref, int_sem.at[1]),
    ]
    for c in ints:
        c.start()
    whole = [
        pltpu.make_async_copy(blocks_hbm.at[g], blocks.at[g], block_sem.at[g]) for g in range(SLOTS)
    ]
    for c in whole:
        c.start()
    wide[...] = jnp.zeros_like(wide)
    for c in ints:
        c.wait()
    copies = []
    for g in range(SLOTS):
        slot = here * SLOTS + g
        row = pl.multiple_of(index_ref[0, slot] * BW, BW)
        col = pl.multiple_of(index_ref[1, slot] * BW, BW)
        group = [
            pltpu.make_async_copy(inactive_hbm.at[:, pl.ds(row, BW)], ina_row.at[g], ir_sem.at[g]),
            pltpu.make_async_copy(inactive_hbm.at[:, pl.ds(col, BW)], ina_col.at[g], ic_sem.at[g]),
            pltpu.make_async_copy(active_hbm.at[:, pl.ds(row, BW)], act_row.at[g], ar_sem.at[g]),
            pltpu.make_async_copy(active_hbm.at[:, pl.ds(col, BW)], act_col.at[g], ac_sem.at[g]),
        ]
        for c in group:
            c.start()
        copies.append(group + [whole[g]])
    for g in range(SLOTS):
        live = mask_ref[here * SLOTS + g].astype(F32)
        for c in copies[g]:
            c.wait()
        density = lax.dot_general(
            ina_row[g], ina_col[g], (((0,), (0,)), ((), ())), preferred_element_type=F32
        )
        density = density.astype(BF16).astype(F32) * live
        for p in range(ROWS):
            product = blocks[g, p].astype(F32) * density
            part = jnp.sum(product.reshape(BW // 8, 8, BW), axis=0)
            if g == 0:
                sums[p] = part
            else:
                sums[p] = sums[p] + part
        column = act_col[g].astype(F32)
        for p in range(PER):
            wide[pl.ds(ACT * p, ACT), pl.ds(BW * p, BW)] = column
        weights = wide[...].astype(BF16)
        for k in range(GROUPS):
            joined = jnp.concatenate([blocks[g, k * PER + p] for p in range(PER)], axis=1)
            half = nt(joined, weights)
            halves[pl.ds(g * BW, BW), pl.ds(k * BW, BW)] = half.astype(BF16)
    rows = jnp.concatenate(
        [
            act_row[g].astype(F32) * mask_ref[here * SLOTS + g].astype(F32)
            for g in range(SLOTS)
        ],
        axis=1,
    ).astype(BF16)
    fitted = jnp.dot(rows, halves[...], preferred_element_type=F32)
    coupling = jnp.sum(jnp.sum(sums[...], axis=1), axis=1, keepdims=True) * (1.0 / BW)
    coupling = jnp.concatenate([coupling, jnp.zeros((ACT - ROWS, 1), F32)], axis=0)
    high = coupling.astype(BF16).astype(F32)
    low = coupling - high
    spare = lanes((ACT, BW)) >= USED
    for k in range(GROUPS):
        tail = high if k == 0 else low if k == 1 else jnp.zeros_like(high)
        tile = jnp.where(spare, jnp.broadcast_to(tail, (ACT, BW)), fitted[:, k * BW : (k + 1) * BW])
        out_ref[:, pl.ds(k * BW, BW)] = tile.astype(BF16)


def expand_kernel(
    own_ref, one_ref, two_ref, three_ref, blocks, keep_ref, send_ref,
    coupling_ref, spread, left, coulomb, main, rest,
):
    here = lax.axis_index("pair")
    core = lax.axis_index("core")
    total = (own_ref[...].astype(F32) + two_ref[...].astype(F32)) + (
        one_ref[...].astype(F32) + three_ref[...].astype(F32)
    )
    both = total[:, :BW] + total[:, BW : 2 * BW]
    coupling = jnp.sum(jnp.where(lanes((ACT, BW)) == USED, both, 0.0), axis=1, keepdims=True)
    coupling_ref[...] = jnp.broadcast_to(coupling.astype(BF16).astype(F32), (ACT, BW))
    fitted = total.astype(BF16).astype(F32)
    offset = lanes((ACT, BW)) - sublanes((ACT, BW))
    keep = offset == 0
    for p in range(1, PER):
        keep = keep | (offset == ACT * p)
    keep = jnp.concatenate([keep.astype(F32)] * GROUPS, axis=1)
    for t in range(0, ACT, 2):
        pair = jnp.concatenate(
            [jnp.broadcast_to(fitted[t + d : t + d + 1, :], keep.shape) * keep for d in range(2)],
            axis=0,
        )
        spread[pl.ds(t * ACT, 2 * ACT), :] = pair.astype(BF16)
    shape = (GROUPS * BW, BW)
    lane = lanes(shape)
    group = (
        (lane >= PER).astype(jnp.int32)
        + (lane >= 2 * PER).astype(jnp.int32)
        + (lane >= 3 * PER).astype(jnp.int32)
    )
    start = group * BW + (lane - group * PER) * ACT
    position = sublanes(shape) - start
    pick = (position >= 0) & (position < ACT) & (lane < ROWS)
    folded = jnp.dot(
        spread[...], pick.astype(F32).astype(BF16), preferred_element_type=F32
    ).astype(BF16)
    left[...] = folded
    columns = left[pl.ds(pl.multiple_of(here * BW, BW), BW), :]
    tail = left[pl.ds(4 * BW, PAIRS - 4 * BW), :]
    main[...] = nt(folded, columns)
    rest[...] = nt(folded, jnp.concatenate([tail, tail], axis=0))
    for g in range(SLOTS):
        total_g = jnp.zeros((BW, BW), F32)
        for p in range(ROWS):
            factor = jnp.broadcast_to(coupling_ref[pl.ds(p, 1), :], (BW, BW))
            total_g = total_g + blocks[g, p].astype(F32) * factor
        coulomb[pl.ds(g * BW, BW), :] = total_g
    low_lane = lanes((CHIPS, BW)) < BW // 2
    for ref, which in ((keep_ref, core), (send_ref, 1 - core)):
        for x in range(NX):
            for z in range(NZ):
                row = pl.multiple_of(z // 2 * BW + 32 * x + 16 * which + 8 * (z % 2), 8)
                ref[pl.ds((x * NZ + z) * MSG, 8), :] = coulomb[pl.ds(row, 8), :]
        for s in range(9):
            ref[pl.ds(8 + s, CHIPS, stride=MSG), :] = main[pl.ds(9 * which + s, CHIPS, stride=18), :]
        for s in range(7):
            value = rest[pl.ds(9 * which + s, CHIPS, stride=18), :]
            if s < 2:
                other = rest[pl.ds(9 * which + 7 + s, CHIPS, stride=18), :]
                value = jnp.where(low_lane, value, other)
            ref[pl.ds(17 + s, CHIPS, stride=MSG), :] = value


def along_x_kernel(parts_ref, out_ref):
    total = jnp.sum(parts_ref[...].astype(F32), axis=0)
    pieces = [total[z * MSG : (z + 1) * MSG] for z in range(NZ)]
    fock = jnp.concatenate([p[0:8] for p in pieces], axis=0).astype(BF16)
    for z in range(NZ):
        out_ref[z, 0:64, :] = fock
        out_ref[z, 64:80, :] = pieces[z][8:MSG].astype(BF16)


def route_kernel(mask_ref, owner_ref, parts_ref, out_ref, tile):
    here = lax.axis_index("pair")
    total = jnp.sum(parts_ref[...].astype(F32), axis=0)
    gram = total[64:80] * (1.0 / AUX)
    high = gram.astype(BF16)
    low = (gram - high.astype(F32)).astype(BF16)
    scaled = total[0:64] * (1.0 / math.sqrt(AUX))
    tile[...] = jnp.zeros_like(tile)
    for o in range(OWNERS):
        place = jnp.int32(0)
        for g in range(SLOTS):
            slot = here * SLOTS + g
            chosen = (mask_ref[slot] == 1) & (owner_ref[slot] == o)

            @pl.when(chosen & (place < 2))
            def _(o=o, g=g, place=place):
                tile[o, pl.ds(pl.multiple_of(16 * place, 16), 16), :] = scaled[16 * g : 16 * g + 16]

            place = place + chosen.astype(jnp.int32)
    for o in range(OWNERS):
        piece = tile[o].astype(BF16)
        for x in range(NX):
            out_ref[o * NX + x, 0:32, :] = piece
            out_ref[o * NX + x, 32:48, :] = high
            out_ref[o * NX + x, 48:64, :] = low


def place_kernel(mask_ref, owner_ref, own_ref, other_ref, fock_ref, gram_ref):
    here = lax.axis_index("pair")
    core = lax.axis_index("core")
    along = lax.axis_index("x")
    fock_ref[...] = jnp.zeros_like(fock_ref)
    rank = jnp.int32(0)
    for q in range(OWNERS):
        place = jnp.int32(0)
        for g in range(SLOTS):
            slot = q * SLOTS + g
            chosen = (mask_ref[slot] == 1) & (owner_ref[slot] == here)

            @pl.when(chosen & (place < 2))
            def _(q=q, rank=rank, place=place):
                source = pl.ds(pl.multiple_of(16 * place, 16), 16)
                for n, ref in enumerate((own_ref, other_ref)):
                    which = core if n == 0 else 1 - core
                    for x in range(NX):
                        row = pl.multiple_of(rank * BW + 32 * x + 16 * which, 16)
                        fock_ref[pl.ds(row, 16), :] = ref[q * NX + x, source, :].astype(F32)

            place = place + chosen.astype(jnp.int32)
            rank = rank + chosen.astype(jnp.int32)
    for q in range(OWNERS):
        high = own_ref[q * NX + along, 32:48, :].astype(F32)
        low = own_ref[q * NX + along, 48:64, :].astype(F32)
        gram = high + low
        gram_ref[:, q * BW : (q + 1) * BW] = gram[0:9]
        if q == 0:
            gram_ref[0:7, 4 * BW : PAIRS] = gram[9:16, 0 : BW // 2]
            gram_ref[7:9, 4 * BW : PAIRS] = gram[9:11, BW // 2 : BW]


def from_others(x):
    return [
        lax.ppermute(x, "pair", [(i, (i + s) % OWNERS) for i in range(OWNERS)])
        for s in range(1, OWNERS)
    ]


def shards(three_centre, block_mask, block_owner, block_index, active_orbitals, inactive_orbitals):
    dma = pltpu.SemaphoreType.DMA
    pinned = [
        pltpu.with_memory_space_constraint(a, pltpu.HBM)
        for a in (block_mask, block_index, three_centre, active_orbitals, inactive_orbitals)
    ]
    message, blocks = pl.pallas_call(
        contract_kernel,
        out_shape=[
            pltpu.VMEM((ACT, GROUPS * BW), BF16),
            pltpu.VMEM((SLOTS, ROWS, BW, BW), BF16),
        ],
        in_specs=[HBM] * 5,
        out_specs=[VMEM, VMEM],
        scratch_shapes=[
            pltpu.SMEM((16,), jnp.int32),
            pltpu.SMEM((2, 16), jnp.int32),
            pltpu.VMEM((SLOTS, ACT, BW), BF16),
            pltpu.VMEM((SLOTS, ACT, BW), BF16),
            pltpu.VMEM((SLOTS, 256, BW), BF16),
            pltpu.VMEM((SLOTS, 256, BW), BF16),
            pltpu.VMEM((BW, PER * BW), F32),
            pltpu.VMEM((SLOTS * BW, GROUPS * BW), BF16),
            pltpu.VMEM((ROWS, 8, BW), F32),
            dma((SLOTS,)), dma((SLOTS,)), dma((SLOTS,)), dma((SLOTS,)), dma((SLOTS,)), dma((2,)),
        ],
        compiler_params=limit(8192),
        name="contract",
    )(*pinned)
    one, two, three = from_others(message)
    rows = CHIPS * MSG
    keep, send = pl.pallas_call(
        expand_kernel,
        out_shape=[pltpu.VMEM((rows, BW), F32)] * 2,
        in_specs=[VMEM] * 5,
        out_specs=[VMEM, VMEM],
        scratch_shapes=[
            pltpu.VMEM((ACT, BW), F32),
            pltpu.VMEM((PAIRS, GROUPS * BW), BF16),
            pltpu.VMEM((PAIRS, BW), BF16),
            pltpu.VMEM((SLOTS * BW, BW), F32),
            pltpu.VMEM((PAIRS, BW), F32),
            pltpu.VMEM((PAIRS, BW), F32),
        ],
        compiler_params=limit(8192),
        name="expand",
    )(message, one, two, three, blocks)
    swap = [(0, 1), (1, 0)]
    chip_sum = (keep + lax.ppermute(send, "core", swap)).astype(BF16)
    along_x = lax.all_to_all(chip_sum.reshape(NX, NZ * MSG, BW), "x", 0, 0, tiled=True)
    pieces = pl.pallas_call(
        along_x_kernel,
        out_shape=pltpu.VMEM((NZ, 80, BW), BF16),
        in_specs=[VMEM],
        out_specs=VMEM,
        compiler_params=limit(4096),
        name="along_x",
    )(along_x)
    along_z = lax.all_to_all(pieces, "z", 0, 0, tiled=True)
    pieces = pl.pallas_call(
        route_kernel,
        out_shape=pltpu.VMEM((OWNERS * NX, 64, BW), BF16),
        in_specs=[SMEM, SMEM, VMEM],
        out_specs=VMEM,
        scratch_shapes=[pltpu.VMEM((OWNERS, 32, BW), F32)],
        compiler_params=limit(4096),
        name="route",
    )(block_mask, block_owner, along_z)
    received = lax.all_to_all(pieces, ("pair", "x"), 0, 0, tiled=True)
    partner = lax.ppermute(received, "core", swap)
    fock, integrals = pl.pallas_call(
        place_kernel,
        out_shape=[
            jax.ShapeDtypeStruct((8 * BW, BW), F32),
            jax.ShapeDtypeStruct((9, PAIRS), F32),
        ],
        in_specs=[SMEM, SMEM, VMEM, VMEM],
        out_specs=[VMEM, VMEM],
        compiler_params=limit(4096),
        name="place",
    )(block_mask, block_owner, received, partner)
    return (fock.reshape(8, BW, BW), integrals)


def solution(mesh):
    split = Mesh(mesh.devices.reshape(NX, NZ, CORES, OWNERS), ("x", "z", "core", "pair"))
    aux = ("x", "z", "core")
    return jax.shard_map(
        shards,
        mesh=split,
        in_specs=(P("pair", aux, None, None), P(), P(), P(), P(), P()),
        out_specs=(P("pair", None, None), P(aux, None)),
        check_vma=False,
    )
```

```python
import math

import jax
import jax.numpy as jnp
from jax import lax
from jax.experimental import pallas as pl
from jax.experimental.pallas import tpu as pltpu
from jax.sharding import Mesh, PartitionSpec as P

SLOTS = 4
ROWS = 20
BW = 128
ACT = 24
PAIRS = 576
GROUPS = 4
PER = 5
USED = PER * ACT
NX = 4
NZ = 8
CHIPS = NX * NZ
CORES = 2
OWNERS = 4
AUX = 1280
NIN = 256
NAO = 3072
MSG = 24
F32 = jnp.float32
BF16 = jnp.bfloat16

HBM = pl.BlockSpec(memory_space=pltpu.HBM)
VMEM = pl.BlockSpec(memory_space=pltpu.VMEM)


def limit(kib):
    return pltpu.CompilerParams(vmem_limit_bytes=kib << 10)


def nt(a, b):
    return lax.dot_general(a, b, (((1,), (1,)), ((), ())), preferred_element_type=F32)


def lanes(shape):
    return lax.broadcasted_iota(jnp.int32, shape, len(shape) - 1)


def sublanes(shape):
    return lax.broadcasted_iota(jnp.int32, shape, len(shape) - 2)


def contract_kernel(
    mask_hbm, owner_hbm, index_hbm, blocks_hbm, active_hbm, inactive_hbm,
    out_ref, blocks, route_ref, place_ref,
    mask_ref, owner_ref, index_ref, active, inactive, wide, halves, density, sums,
    int_sem, ina_sem, act_sem, block_sem,
):
    here = lax.axis_index("pair")
    ints = [
        pltpu.make_async_copy(index_hbm, index_ref, int_sem.at[0]),
        pltpu.make_async_copy(mask_hbm, mask_ref, int_sem.at[1]),
        pltpu.make_async_copy(owner_hbm, owner_ref, int_sem.at[2]),
    ]
    part = NIN // SLOTS
    inactives = [
        pltpu.make_async_copy(
            inactive_hbm.at[pl.ds(n * part, part)], inactive.at[pl.ds(n * part, part)], ina_sem.at[n]
        )
        for n in range(SLOTS)
    ]
    actives = [pltpu.make_async_copy(active_hbm, active, act_sem.at[0])]
    whole = [
        pltpu.make_async_copy(blocks_hbm.at[g], blocks.at[g], block_sem.at[g]) for g in range(SLOTS)
    ]
    for c in ints + inactives + actives + whole:
        c.start()
    wide[...] = jnp.zeros_like(wide)
    for c in ints:
        c.wait()
    lives = [mask_ref[here * SLOTS + g] for g in range(SLOTS)]
    owners = [owner_ref[here * SLOTS + g] for g in range(SLOTS)]
    rows = [pl.multiple_of(index_ref[0, here * SLOTS + g] * BW, BW) for g in range(SLOTS)]
    cols = [pl.multiple_of(index_ref[1, here * SLOTS + g] * BW, BW) for g in range(SLOTS)]
    col = lanes((1, BW))
    at = sublanes((BW, BW))
    target = jnp.full((1, BW), -BW, jnp.int32)
    for g in range(SLOTS):
        place = jnp.int32(0)
        for h in range(g):
            place = place + jnp.where((lives[h] == 1) & (owners[h] == owners[g]), 1, 0)
        first = jnp.where(lives[g] == 1, 16 * (2 * owners[g] + place), -BW)
        inside = (col >= 16 * g) & (col < 16 * (g + 1))
        target = jnp.where(inside, first + col - 16 * g, target)
    route_ref[...] = (at == target).astype(F32).astype(BF16)
    target = jnp.full((1, BW), -BW, jnp.int32)
    rank = jnp.int32(0)
    for q in range(OWNERS):
        place = jnp.int32(0)
        firsts = [jnp.int32(-BW)] * 2
        for g in range(SLOTS):
            slot = q * SLOTS + g
            chosen = (mask_ref[slot] == 1) & (owner_ref[slot] == here)
            firsts = [jnp.where(chosen & (place == k), 16 * rank, f) for k, f in enumerate(firsts)]
            place = place + jnp.where(chosen, 1, 0)
            rank = rank + jnp.where(chosen, 1, 0)
        for k in range(2):
            begin = 16 * (2 * q + k)
            inside = (col >= begin) & (col < begin + 16)
            target = jnp.where(inside, firsts[k] + col - begin, target)
    place_ref[...] = (at == target).astype(F32).astype(BF16)
    for c in inactives:
        c.wait()
    for g in range(SLOTS):
        square = lax.dot_general(
            inactive[:, pl.ds(rows[g], BW)],
            inactive[:, pl.ds(cols[g], BW)],
            (((0,), (0,)), ((), ())),
            preferred_element_type=F32,
        )
        density[g] = square.astype(BF16).astype(F32) * lives[g].astype(F32)
    actives[0].wait()
    for g in range(SLOTS):
        column = active[:, pl.ds(cols[g], BW)].astype(F32)
        for p in range(PER):
            wide[pl.ds(ACT * p, ACT), pl.ds(BW * p, BW)] = column
        weights = wide[...].astype(BF16)
        whole[g].wait()
        for k in range(GROUPS):
            joined = jnp.concatenate([blocks[g, k * PER + p] for p in range(PER)], axis=1)
            half = nt(joined, weights)
            halves[pl.ds(g * BW, BW), pl.ds(k * BW, BW)] = half.astype(BF16)
        square = density[g]
        for p in range(ROWS):
            product = blocks[g, p].astype(F32) * square
            part_sum = jnp.sum(product.reshape(BW // 8, 8, BW), axis=0)
            if g == 0:
                sums[p] = part_sum
            else:
                sums[p] = sums[p] + part_sum
    left_side = jnp.concatenate(
        [active[:, pl.ds(rows[g], BW)].astype(F32) * lives[g].astype(F32) for g in range(SLOTS)],
        axis=1,
    ).astype(BF16)
    fitted = jnp.dot(left_side, halves[...], preferred_element_type=F32)
    coupling = jnp.sum(jnp.sum(sums[...], axis=1), axis=1, keepdims=True) * (1.0 / BW)
    coupling = jnp.concatenate([coupling, jnp.zeros((ACT - ROWS, 1), F32)], axis=0)
    high = coupling.astype(BF16).astype(F32)
    low = coupling - high
    spare = lanes((ACT, BW)) >= USED
    for k in range(GROUPS):
        tail = high if k == 0 else low if k == 1 else jnp.zeros_like(high)
        tile = jnp.where(spare, jnp.broadcast_to(tail, (ACT, BW)), fitted[:, k * BW : (k + 1) * BW])
        out_ref[:, pl.ds(k * BW, BW)] = tile.astype(BF16)


def expand_kernel(
    own_ref, one_ref, two_ref, three_ref, blocks, keep_ref, send_ref,
    coupling_ref, spread, left, coulomb, main, rest,
):
    here = lax.axis_index("pair")
    core = lax.axis_index("core")
    along = lax.axis_index("x")
    total = (own_ref[...].astype(F32) + two_ref[...].astype(F32)) + (
        one_ref[...].astype(F32) + three_ref[...].astype(F32)
    )
    both = total[:, :BW] + total[:, BW : 2 * BW]
    coupling = jnp.sum(jnp.where(lanes((ACT, BW)) == USED, both, 0.0), axis=1, keepdims=True)
    coupling_ref[...] = jnp.broadcast_to(coupling.astype(BF16).astype(F32), (ACT, BW))
    fitted = total.astype(BF16).astype(F32)
    offset = lanes((ACT, BW)) - sublanes((ACT, BW))
    keep = offset == 0
    for p in range(1, PER):
        keep = keep | (offset == ACT * p)
    keep = jnp.concatenate([keep.astype(F32)] * GROUPS, axis=1)
    for t in range(0, ACT, 2):
        pair = jnp.concatenate(
            [jnp.broadcast_to(fitted[t + d : t + d + 1, :], keep.shape) * keep for d in range(2)],
            axis=0,
        )
        spread[pl.ds(t * ACT, 2 * ACT), :] = pair.astype(BF16)
    shape = (GROUPS * BW, BW)
    lane = lanes(shape)
    group = (
        (lane >= PER).astype(jnp.int32)
        + (lane >= 2 * PER).astype(jnp.int32)
        + (lane >= 3 * PER).astype(jnp.int32)
    )
    start = group * BW + (lane - group * PER) * ACT
    position = sublanes(shape) - start
    pick = (position >= 0) & (position < ACT) & (lane < ROWS)
    folded = jnp.dot(
        spread[...], pick.astype(F32).astype(BF16), preferred_element_type=F32
    ).astype(BF16)
    left[...] = folded
    columns = left[pl.ds(pl.multiple_of(here * BW, BW), BW), :]
    tail = left[pl.ds(4 * BW, PAIRS - 4 * BW), :]
    main[...] = nt(folded, columns)
    rest[...] = nt(folded, jnp.concatenate([tail, tail], axis=0))
    for g in range(SLOTS):
        total_g = jnp.zeros((BW, BW), F32)
        for p in range(ROWS):
            factor = jnp.broadcast_to(coupling_ref[pl.ds(p, 1), :], (BW, BW))
            total_g = total_g + blocks[g, p].astype(F32) * factor
        coulomb[pl.ds(g * BW, BW), :] = total_g
    low_lane = lanes((NZ, BW)) < BW // 2
    for ref, which in ((keep_ref, core), (send_ref, 1 - core)):
        for step in range(NX):
            x = lax.rem(along + step, NX)
            base = step * NZ * MSG
            for z in range(NZ):
                row = pl.multiple_of(z // 2 * BW + 32 * x + 16 * which + 8 * (z % 2), 8)
                ref[pl.ds(base + z * MSG, 8), :] = coulomb[pl.ds(row, 8), :]
            first = 144 * x + 9 * which
            for s in range(9):
                ref[pl.ds(base + 8 + s, NZ, stride=MSG), :] = main[pl.ds(first + s, NZ, stride=18), :]
            for s in range(7):
                value = rest[pl.ds(first + s, NZ, stride=18), :]
                if s < 2:
                    other = rest[pl.ds(first + 7 + s, NZ, stride=18), :]
                    value = jnp.where(low_lane, value, other)
                ref[pl.ds(base + 17 + s, NZ, stride=MSG), :] = value


def along_x_kernel(own_ref, one_ref, two_ref, three_ref, out_ref):
    total = own_ref[...]
    for ref in (one_ref, two_ref, three_ref):
        total = total + ref[...].astype(F32)
    pieces = [total[z * MSG : (z + 1) * MSG] for z in range(NZ)]
    fock = jnp.concatenate([p[0:8] for p in pieces], axis=0).astype(BF16)
    for z in range(NZ):
        out_ref[z, 0:64, :] = fock
        out_ref[z, 64:80, :] = pieces[z][8:MSG].astype(BF16)


def route_kernel(route_ref, parts_ref, out_ref):
    total = jnp.sum(parts_ref[...].astype(F32), axis=0)
    gram = (total[64:80] * (1.0 / AUX)).astype(BF16)
    scaled = total[0:64] * (1.0 / math.sqrt(AUX))
    scaled = jnp.concatenate([scaled, jnp.zeros_like(scaled)], axis=0).astype(BF16)
    chosen = jnp.dot(route_ref[...], scaled, preferred_element_type=F32).astype(BF16)
    for o in range(OWNERS):
        for x in range(NX):
            out_ref[o * NX + x, 0:32, :] = chosen[32 * o : 32 * (o + 1)]
            out_ref[o * NX + x, 32:48, :] = gram


def place_kernel(place_ref, own_ref, other_ref, fock_ref, gram_ref):
    core = lax.axis_index("core")
    along = lax.axis_index("x")
    table = place_ref[...]
    for n, ref in enumerate((own_ref, other_ref)):
        which = core if n == 0 else 1 - core
        for x in range(NX):
            pieces = jnp.concatenate([ref[q * NX + x, 0:32, :] for q in range(OWNERS)], axis=0)
            placed = jnp.dot(table, pieces, preferred_element_type=F32)
            for rank in range(8):
                row = pl.multiple_of(rank * BW + 32 * x + 16 * which, 16)
                fock_ref[pl.ds(row, 16), :] = placed[16 * rank : 16 * (rank + 1)]
    for q in range(OWNERS):
        gram = own_ref[q * NX + along, 32:48, :].astype(F32)
        gram_ref[:, q * BW : (q + 1) * BW] = gram[0:9]
        if q == 0:
            gram_ref[0:7, 4 * BW : PAIRS] = gram[9:16, 0 : BW // 2]
            gram_ref[7:9, 4 * BW : PAIRS] = gram[9:11, BW // 2 : BW]


def from_others(x, axis="pair"):
    return [
        lax.ppermute(x if axis == "pair" else x[s], axis, [(i, (i + s) % 4) for i in range(4)])
        for s in range(1, 4)
    ]


def shards(three_centre, block_mask, block_owner, block_index, active_orbitals, inactive_orbitals):
    dma = pltpu.SemaphoreType.DMA
    inputs = (
        block_mask, block_owner, block_index, three_centre, active_orbitals, inactive_orbitals
    )
    pinned = [pltpu.with_memory_space_constraint(a, pltpu.HBM) for a in inputs]
    message, blocks, routes, places = pl.pallas_call(
        contract_kernel,
        out_shape=[
            pltpu.VMEM((ACT, GROUPS * BW), BF16),
            pltpu.VMEM((SLOTS, ROWS, BW, BW), BF16),
            pltpu.VMEM((BW, BW), BF16),
            pltpu.VMEM((BW, BW), BF16),
        ],
        in_specs=[HBM] * 6,
        out_specs=[VMEM] * 4,
        scratch_shapes=[
            pltpu.SMEM((16,), jnp.int32),
            pltpu.SMEM((16,), jnp.int32),
            pltpu.SMEM((2, 16), jnp.int32),
            pltpu.VMEM((ACT, NAO), BF16),
            pltpu.VMEM((NIN, NAO), BF16),
            pltpu.VMEM((BW, PER * BW), F32),
            pltpu.VMEM((SLOTS * BW, GROUPS * BW), BF16),
            pltpu.VMEM((SLOTS, BW, BW), F32),
            pltpu.VMEM((ROWS, 8, BW), F32),
            dma((3,)), dma((SLOTS,)), dma((1,)), dma((SLOTS,)),
        ],
        compiler_params=limit(8192),
        name="contract",
    )(*pinned)
    one, two, three = from_others(message)
    rows = CHIPS * MSG
    keep, send = pl.pallas_call(
        expand_kernel,
        out_shape=[pltpu.VMEM((rows, BW), F32)] * 2,
        in_specs=[VMEM] * 5,
        out_specs=[VMEM, VMEM],
        scratch_shapes=[
            pltpu.VMEM((ACT, BW), F32),
            pltpu.VMEM((PAIRS, GROUPS * BW), BF16),
            pltpu.VMEM((PAIRS, BW), BF16),
            pltpu.VMEM((SLOTS * BW, BW), F32),
            pltpu.VMEM((PAIRS, BW), F32),
            pltpu.VMEM((PAIRS, BW), F32),
        ],
        compiler_params=limit(8192),
        name="expand",
    )(message, one, two, three, blocks)
    swap = [(0, 1), (1, 0)]
    chip_sum = (keep + lax.ppermute(send, "core", swap)).reshape(NX, NZ * MSG, BW)
    one, two, three = from_others(chip_sum.astype(BF16), "x")
    pieces = pl.pallas_call(
        along_x_kernel,
        out_shape=pltpu.VMEM((NZ, 80, BW), BF16),
        in_specs=[VMEM] * 4,
        out_specs=VMEM,
        compiler_params=limit(4096),
        name="along_x",
    )(chip_sum[0], one, two, three)
    along_z = lax.all_to_all(pieces, "z", 0, 0, tiled=True)
    pieces = pl.pallas_call(
        route_kernel,
        out_shape=pltpu.VMEM((OWNERS * NX, 48, BW), BF16),
        in_specs=[VMEM] * 2,
        out_specs=VMEM,
        compiler_params=limit(4096),
        name="route",
    )(routes, along_z)
    received = lax.all_to_all(pieces, ("pair", "x"), 0, 0, tiled=True)
    partner = lax.ppermute(received, "core", swap)
    fock, integrals = pl.pallas_call(
        place_kernel,
        out_shape=[
            jax.ShapeDtypeStruct((8 * BW, BW), F32),
            jax.ShapeDtypeStruct((9, PAIRS), F32),
        ],
        in_specs=[VMEM] * 3,
        out_specs=[VMEM, VMEM],
        compiler_params=limit(4096),
        name="place",
    )(places, received, partner)
    return (fock.reshape(8, BW, BW), integrals)


def solution(mesh):
    split = Mesh(mesh.devices.reshape(NX, NZ, CORES, OWNERS), ("x", "z", "core", "pair"))
    aux = ("x", "z", "core")
    return jax.shard_map(
        shards,
        mesh=split,
        in_specs=(P("pair", aux, None, None), P(), P(), P(), P(), P()),
        out_specs=(P("pair", None, None), P(aux, None)),
        check_vma=False,
    )
```

```python
import math

import jax
import jax.numpy as jnp
from jax import lax
from jax.experimental import pallas as pl
from jax.experimental.pallas import tpu as pltpu
from jax.sharding import Mesh, PartitionSpec as P

SLOTS = 4
ROWS = 20
BW = 128
ACT = 24
PAIRS = 576
GROUPS = 4
PER = 5
USED = PER * ACT
NX = 4
NZ = 8
CHIPS = NX * NZ
CORES = 2
OWNERS = 4
AUX = 1280
NIN = 256
NAO = 3072
MSG = 24
F32 = jnp.float32
BF16 = jnp.bfloat16

HBM = pl.BlockSpec(memory_space=pltpu.HBM)
VMEM = pl.BlockSpec(memory_space=pltpu.VMEM)


def limit(kib):
    return pltpu.CompilerParams(vmem_limit_bytes=kib << 10)


def nt(a, b):
    return lax.dot_general(a, b, (((1,), (1,)), ((), ())), preferred_element_type=F32)


def lanes(shape):
    return lax.broadcasted_iota(jnp.int32, shape, len(shape) - 1)


def sublanes(shape):
    return lax.broadcasted_iota(jnp.int32, shape, len(shape) - 2)


def contract_kernel(
    mask_hbm, owner_hbm, index_hbm, blocks_hbm, active_hbm, inactive_hbm,
    out_ref, blocks, route_ref, place_ref, keep_mask, pick_mask,
    mask_ref, owner_ref, index_ref, active, inactive, wide, halves, density, sums,
    int_sem, ina_sem, act_sem, block_sem,
):
    here = lax.axis_index("pair")
    ints = [
        pltpu.make_async_copy(index_hbm, index_ref, int_sem.at[0]),
        pltpu.make_async_copy(mask_hbm, mask_ref, int_sem.at[1]),
        pltpu.make_async_copy(owner_hbm, owner_ref, int_sem.at[2]),
    ]
    part = NIN // SLOTS
    inactives = [
        pltpu.make_async_copy(
            inactive_hbm.at[pl.ds(n * part, part)], inactive.at[pl.ds(n * part, part)], ina_sem.at[n]
        )
        for n in range(SLOTS)
    ]
    actives = [pltpu.make_async_copy(active_hbm, active, act_sem.at[0])]
    whole = [
        pltpu.make_async_copy(blocks_hbm.at[g], blocks.at[g], block_sem.at[g]) for g in range(SLOTS)
    ]
    for c in ints + inactives + actives:
        c.start()
    for c in whole:
        c.start(priority=1)
    wide[...] = jnp.zeros_like(wide)
    offset = lanes((ACT, BW)) - sublanes((ACT, BW))
    keep = offset == 0
    for p in range(1, PER):
        keep = keep | (offset == ACT * p)
    keep = jnp.concatenate([keep.astype(F32)] * GROUPS, axis=1)
    keep_mask[...] = keep
    shape = (GROUPS * BW, BW)
    lane = lanes(shape)
    group = (
        (lane >= PER).astype(jnp.int32)
        + (lane >= 2 * PER).astype(jnp.int32)
        + (lane >= 3 * PER).astype(jnp.int32)
    )
    start = group * BW + (lane - group * PER) * ACT
    position = sublanes(shape) - start
    pick = (position >= 0) & (position < ACT) & (lane < ROWS)
    pick_mask[...] = pick.astype(F32).astype(BF16)
    for c in ints:
        c.wait()
    lives = [mask_ref[here * SLOTS + g] for g in range(SLOTS)]
    owners = [owner_ref[here * SLOTS + g] for g in range(SLOTS)]
    rows = [pl.multiple_of(index_ref[0, here * SLOTS + g] * BW, BW) for g in range(SLOTS)]
    cols = [pl.multiple_of(index_ref[1, here * SLOTS + g] * BW, BW) for g in range(SLOTS)]
    col = lanes((1, BW))
    at = sublanes((BW, BW))
    target = jnp.full((1, BW), -BW, jnp.int32)
    for g in range(SLOTS):
        place = jnp.int32(0)
        for h in range(g):
            place = place + jnp.where((lives[h] == 1) & (owners[h] == owners[g]), 1, 0)
        first = jnp.where(lives[g] == 1, 16 * (2 * owners[g] + place), -BW)
        inside = (col >= 16 * g) & (col < 16 * (g + 1))
        target = jnp.where(inside, first + col - 16 * g, target)
    route_ref[...] = (at == target).astype(F32).astype(BF16)
    target = jnp.full((1, BW), -BW, jnp.int32)
    rank = jnp.int32(0)
    for q in range(OWNERS):
        place = jnp.int32(0)
        firsts = [jnp.int32(-BW)] * 2
        for g in range(SLOTS):
            slot = q * SLOTS + g
            chosen = (mask_ref[slot] == 1) & (owner_ref[slot] == here)
            firsts = [jnp.where(chosen & (place == k), 16 * rank, f) for k, f in enumerate(firsts)]
            place = place + jnp.where(chosen, 1, 0)
            rank = rank + jnp.where(chosen, 1, 0)
        for k in range(2):
            begin = 16 * (2 * q + k)
            inside = (col >= begin) & (col < begin + 16)
            target = jnp.where(inside, firsts[k] + col - begin, target)
    place_ref[...] = (at == target).astype(F32).astype(BF16)
    for c in inactives:
        c.wait()
    for g in range(SLOTS):
        square = lax.dot_general(
            inactive[:, pl.ds(rows[g], BW)],
            inactive[:, pl.ds(cols[g], BW)],
            (((0,), (0,)), ((), ())),
            preferred_element_type=F32,
        )
        density[g] = square.astype(BF16).astype(F32) * lives[g].astype(F32)
    actives[0].wait()
    for g in range(SLOTS):
        column = active[:, pl.ds(cols[g], BW)].astype(F32)
        for p in range(PER):
            wide[pl.ds(ACT * p, ACT), pl.ds(BW * p, BW)] = column
        weights = wide[...].astype(BF16)
        whole[g].wait()
        for k in range(GROUPS):
            joined = jnp.concatenate([blocks[g, k * PER + p] for p in range(PER)], axis=1)
            half = nt(joined, weights)
            halves[pl.ds(g * BW, BW), pl.ds(k * BW, BW)] = half.astype(BF16)
        square = density[g]
        for p in range(ROWS):
            product = blocks[g, p].astype(F32) * square
            part_sum = jnp.sum(product.reshape(BW // 8, 8, BW), axis=0)
            if g == 0:
                sums[p] = part_sum
            else:
                sums[p] = sums[p] + part_sum
    left_side = jnp.concatenate(
        [active[:, pl.ds(rows[g], BW)].astype(F32) * lives[g].astype(F32) for g in range(SLOTS)],
        axis=1,
    ).astype(BF16)
    fitted = jnp.dot(left_side, halves[...], preferred_element_type=F32)
    coupling = jnp.sum(jnp.sum(sums[...], axis=1), axis=1, keepdims=True) * (1.0 / BW)
    coupling = jnp.concatenate([coupling, jnp.zeros((ACT - ROWS, 1), F32)], axis=0)
    high = coupling.astype(BF16).astype(F32)
    low = coupling - high
    spare = lanes((ACT, BW)) >= USED
    for k in range(GROUPS):
        tail = high if k == 0 else low if k == 1 else jnp.zeros_like(high)
        tile = jnp.where(spare, jnp.broadcast_to(tail, (ACT, BW)), fitted[:, k * BW : (k + 1) * BW])
        out_ref[:, pl.ds(k * BW, BW)] = tile.astype(BF16)


def expand_kernel(
    own_ref, one_ref, two_ref, three_ref, blocks, keep_mask, pick_mask, keep_ref, send_ref,
    coupling_ref, spread, left, coulomb, main, rest, scaled_eye,
):
    here = lax.axis_index("pair")
    core = lax.axis_index("core")
    along = lax.axis_index("x")
    total = (own_ref[...].astype(F32) + two_ref[...].astype(F32)) + (
        one_ref[...].astype(F32) + three_ref[...].astype(F32)
    )
    both = total[:, :BW] + total[:, BW : 2 * BW]
    coupling = jnp.sum(jnp.where(lanes((ACT, BW)) == USED, both, 0.0), axis=1, keepdims=True)
    coupling_ref[...] = jnp.broadcast_to(coupling.astype(BF16).astype(F32), (ACT, BW))
    fitted = total.astype(BF16).astype(F32)
    keep = keep_mask[...]
    for t in range(0, ACT, 2):
        pair = jnp.concatenate(
            [jnp.broadcast_to(fitted[t + d : t + d + 1, :], keep.shape) * keep for d in range(2)],
            axis=0,
        )
        spread[pl.ds(t * ACT, 2 * ACT), :] = pair.astype(BF16)
    folded = jnp.dot(
        spread[...], pick_mask[...], preferred_element_type=F32
    ).astype(BF16)
    left[...] = folded
    columns = left[pl.ds(pl.multiple_of(here * BW, BW), BW), :]
    tail = left[pl.ds(4 * BW, PAIRS - 4 * BW), :]
    main[...] = nt(folded, columns)
    rest[...] = nt(folded, jnp.concatenate([tail, tail], axis=0))
    eye = (lanes((BW, BW)) == sublanes((BW, BW))).astype(F32)
    for p in range(ROWS):
        factor = jnp.broadcast_to(coupling_ref[pl.ds(p, 1), :], (BW, BW))
        scaled_eye[pl.ds(p * BW, BW), :] = (eye * factor).astype(BF16)
    joined = jnp.concatenate(
        [jnp.concatenate([blocks[g, p] for p in range(ROWS)], axis=1) for g in (0, 1, 2)], axis=0
    )
    coulomb[pl.ds(0 * BW, 3 * BW), :] = jnp.dot(
        joined, scaled_eye[...], preferred_element_type=F32
    )
    for g in (3,):
        total_g = jnp.zeros((BW, BW), F32)
        for p in range(ROWS):
            factor = jnp.broadcast_to(coupling_ref[pl.ds(p, 1), :], (BW, BW))
            total_g = total_g + blocks[g, p].astype(F32) * factor
        coulomb[pl.ds(g * BW, BW), :] = total_g
    low_lane = lanes((NZ, BW)) < BW // 2
    for ref, which in ((keep_ref, core), (send_ref, 1 - core)):
        for step in range(NX):
            x = lax.rem(along + step, NX)
            base = step * NZ * MSG
            for z in range(NZ):
                row = pl.multiple_of(z // 2 * BW + 32 * x + 16 * which + 8 * (z % 2), 8)
                ref[pl.ds(base + z * MSG, 8), :] = coulomb[pl.ds(row, 8), :]
            first = 144 * x + 9 * which
            for s in range(9):
                ref[pl.ds(base + 8 + s, NZ, stride=MSG), :] = main[pl.ds(first + s, NZ, stride=18), :]
            for s in range(7):
                value = rest[pl.ds(first + s, NZ, stride=18), :]
                if s < 2:
                    other = rest[pl.ds(first + 7 + s, NZ, stride=18), :]
                    value = jnp.where(low_lane, value, other)
                ref[pl.ds(base + 17 + s, NZ, stride=MSG), :] = value


def along_x_kernel(own_ref, one_ref, two_ref, three_ref, out_ref):
    total = own_ref[...]
    for ref in (one_ref, two_ref, three_ref):
        total = total + ref[...].astype(F32)
    pieces = [total[z * MSG : (z + 1) * MSG] for z in range(NZ)]
    fock = jnp.concatenate([p[0:8] for p in pieces], axis=0).astype(BF16)
    for z in range(NZ):
        out_ref[z, 0:64, :] = fock
        out_ref[z, 64:80, :] = pieces[z][8:MSG].astype(BF16)


def route_kernel(route_ref, parts_ref, out_ref):
    total = jnp.sum(parts_ref[...].astype(F32), axis=0)
    gram = (total[64:80] * (1.0 / AUX)).astype(BF16)
    scaled = total[0:64] * (1.0 / math.sqrt(AUX))
    scaled = jnp.concatenate([scaled, jnp.zeros_like(scaled)], axis=0).astype(BF16)
    chosen = jnp.dot(route_ref[...], scaled, preferred_element_type=F32).astype(BF16)
    for o in range(OWNERS):
        for x in range(NX):
            out_ref[o * NX + x, 0:32, :] = chosen[32 * o : 32 * (o + 1)]
            out_ref[o * NX + x, 32:48, :] = gram


def place_kernel(place_ref, own_ref, other_ref, fock_ref, gram_ref):
    core = lax.axis_index("core")
    along = lax.axis_index("x")
    table = place_ref[...]
    for n, ref in enumerate((own_ref, other_ref)):
        which = core if n == 0 else 1 - core
        for x in range(NX):
            pieces = jnp.concatenate([ref[q * NX + x, 0:32, :] for q in range(OWNERS)], axis=0)
            placed = jnp.dot(table, pieces, preferred_element_type=F32)
            for rank in range(8):
                row = pl.multiple_of(rank * BW + 32 * x + 16 * which, 16)
                fock_ref[pl.ds(row, 16), :] = placed[16 * rank : 16 * (rank + 1)]
    for q in range(OWNERS):
        gram = own_ref[q * NX + along, 32:48, :].astype(F32)
        gram_ref[:, q * BW : (q + 1) * BW] = gram[0:9]
        if q == 0:
            gram_ref[0:7, 4 * BW : PAIRS] = gram[9:16, 0 : BW // 2]
            gram_ref[7:9, 4 * BW : PAIRS] = gram[9:11, BW // 2 : BW]


def from_others(x, axis="pair"):
    return [
        lax.ppermute(x if axis == "pair" else x[s], axis, [(i, (i + s) % 4) for i in range(4)])
        for s in range(1, 4)
    ]


def shards(three_centre, block_mask, block_owner, block_index, active_orbitals, inactive_orbitals):
    dma = pltpu.SemaphoreType.DMA
    inputs = (
        block_mask, block_owner, block_index, three_centre, active_orbitals, inactive_orbitals
    )
    pinned = [pltpu.with_memory_space_constraint(a, pltpu.HBM) for a in inputs]
    message, blocks, routes, places, keep_mask, pick_mask = pl.pallas_call(
        contract_kernel,
        out_shape=[
            pltpu.VMEM((ACT, GROUPS * BW), BF16),
            pltpu.VMEM((SLOTS, ROWS, BW, BW), BF16),
            pltpu.VMEM((BW, BW), BF16),
            pltpu.VMEM((BW, BW), BF16),
            pltpu.VMEM((ACT, GROUPS * BW), F32),
            pltpu.VMEM((GROUPS * BW, BW), BF16),
        ],
        in_specs=[HBM] * 6,
        out_specs=[VMEM] * 6,
        scratch_shapes=[
            pltpu.SMEM((16,), jnp.int32),
            pltpu.SMEM((16,), jnp.int32),
            pltpu.SMEM((2, 16), jnp.int32),
            pltpu.VMEM((ACT, NAO), BF16),
            pltpu.VMEM((NIN, NAO), BF16),
            pltpu.VMEM((BW, PER * BW), F32),
            pltpu.VMEM((SLOTS * BW, GROUPS * BW), BF16),
            pltpu.VMEM((SLOTS, BW, BW), F32),
            pltpu.VMEM((ROWS, 8, BW), F32),
            dma((3,)), dma((SLOTS,)), dma((1,)), dma((SLOTS,)),
        ],
        compiler_params=limit(8192),
        name="contract",
    )(*pinned)
    one, two, three = from_others(message)
    rows = CHIPS * MSG
    keep, send = pl.pallas_call(
        expand_kernel,
        out_shape=[pltpu.VMEM((rows, BW), F32)] * 2,
        in_specs=[VMEM] * 7,
        out_specs=[VMEM, VMEM],
        scratch_shapes=[
            pltpu.VMEM((ACT, BW), F32),
            pltpu.VMEM((PAIRS, GROUPS * BW), BF16),
            pltpu.VMEM((PAIRS, BW), BF16),
            pltpu.VMEM((SLOTS * BW, BW), F32),
            pltpu.VMEM((PAIRS, BW), F32),
            pltpu.VMEM((PAIRS, BW), F32),
            pltpu.VMEM((ROWS * BW, BW), BF16),
        ],
        compiler_params=limit(8192),
        name="expand",
    )(message, one, two, three, blocks, keep_mask, pick_mask)
    swap = [(0, 1), (1, 0)]
    chip_sum = (keep + lax.ppermute(send, "core", swap)).reshape(NX, NZ * MSG, BW)
    one, two, three = from_others(chip_sum.astype(BF16), "x")
    pieces = pl.pallas_call(
        along_x_kernel,
        out_shape=pltpu.VMEM((NZ, 80, BW), BF16),
        in_specs=[VMEM] * 4,
        out_specs=VMEM,
        compiler_params=limit(4096),
        name="along_x",
    )(chip_sum[0], one, two, three)
    along_z = lax.all_to_all(pieces, "z", 0, 0, tiled=True)
    pieces = pl.pallas_call(
        route_kernel,
        out_shape=pltpu.VMEM((OWNERS * NX, 48, BW), BF16),
        in_specs=[VMEM] * 2,
        out_specs=VMEM,
        compiler_params=limit(4096),
        name="route",
    )(routes, along_z)
    received = lax.all_to_all(pieces, ("pair", "x"), 0, 0, tiled=True)
    partner = lax.ppermute(received, "core", swap)
    fock, integrals = pl.pallas_call(
        place_kernel,
        out_shape=[
            jax.ShapeDtypeStruct((8 * BW, BW), F32),
            jax.ShapeDtypeStruct((9, PAIRS), F32),
        ],
        in_specs=[VMEM] * 3,
        out_specs=[VMEM, VMEM],
        compiler_params=limit(4096),
        name="place",
    )(places, received, partner)
    return (fock.reshape(8, BW, BW), integrals)


def solution(mesh):
    split = Mesh(mesh.devices.reshape(NX, NZ, CORES, OWNERS), ("x", "z", "core", "pair"))
    aux = ("x", "z", "core")
    return jax.shard_map(
        shards,
        mesh=split,
        in_specs=(P("pair", aux, None, None), P(), P(), P(), P(), P()),
        out_specs=(P("pair", None, None), P(aux, None)),
        check_vma=False,
    )
```

```python
import math

import jax
import jax.numpy as jnp
from jax import lax
from jax.experimental import pallas as pl
from jax.experimental.pallas import tpu as pltpu
from jax.sharding import Mesh, PartitionSpec as P

SLOTS = 4
ROWS = 20
BW = 128
ACT = 24
PAIRS = 576
GROUPS = 4
PER = 5
USED = PER * ACT
NX = 4
NZ = 8
CHIPS = NX * NZ
CORES = 2
OWNERS = 4
AUX = 1280
NIN = 256
NAO = 3072
MSG = 48
F32 = jnp.float32
BF16 = jnp.bfloat16

HBM = pl.BlockSpec(memory_space=pltpu.HBM)
VMEM = pl.BlockSpec(memory_space=pltpu.VMEM)


def limit(kib):
    return pltpu.CompilerParams(vmem_limit_bytes=kib << 10)


def nt(a, b):
    return lax.dot_general(a, b, (((1,), (1,)), ((), ())), preferred_element_type=F32)


def lanes(shape):
    return lax.broadcasted_iota(jnp.int32, shape, len(shape) - 1)


def sublanes(shape):
    return lax.broadcasted_iota(jnp.int32, shape, len(shape) - 2)


def contract_kernel(
    mask_hbm, owner_hbm, index_hbm, blocks_hbm, active_hbm, inactive_hbm,
    out_ref, blocks, route_ref, place_ref, keep_mask, pick_mask,
    mask_ref, owner_ref, index_ref, active, inactive, wide, halves, density, sums,
    int_sem, ina_sem, act_sem, block_sem,
):
    here = lax.axis_index("pair")
    ints = [
        pltpu.make_async_copy(index_hbm, index_ref, int_sem.at[0]),
        pltpu.make_async_copy(mask_hbm, mask_ref, int_sem.at[1]),
        pltpu.make_async_copy(owner_hbm, owner_ref, int_sem.at[2]),
    ]
    part = NIN // SLOTS
    inactives = [
        pltpu.make_async_copy(
            inactive_hbm.at[pl.ds(n * part, part)], inactive.at[pl.ds(n * part, part)], ina_sem.at[n]
        )
        for n in range(SLOTS)
    ]
    actives = [pltpu.make_async_copy(active_hbm, active, act_sem.at[0])]
    whole = [
        pltpu.make_async_copy(blocks_hbm.at[g], blocks.at[g], block_sem.at[g]) for g in range(SLOTS)
    ]
    for c in ints + inactives + actives:
        c.start()
    for c in whole:
        c.start(priority=1)
    wide[...] = jnp.zeros_like(wide)
    offset = lanes((ACT, BW)) - sublanes((ACT, BW))
    keep = offset == 0
    for p in range(1, PER):
        keep = keep | (offset == ACT * p)
    keep = jnp.concatenate([keep.astype(F32)] * GROUPS, axis=1)
    keep_mask[...] = keep
    shape = (GROUPS * BW, BW)
    lane = lanes(shape)
    group = (
        (lane >= PER).astype(jnp.int32)
        + (lane >= 2 * PER).astype(jnp.int32)
        + (lane >= 3 * PER).astype(jnp.int32)
    )
    start = group * BW + (lane - group * PER) * ACT
    position = sublanes(shape) - start
    pick = (position >= 0) & (position < ACT) & (lane < ROWS)
    pick_mask[...] = pick.astype(F32).astype(BF16)
    for c in ints:
        c.wait()
    lives = [mask_ref[here * SLOTS + g] for g in range(SLOTS)]
    owners = [owner_ref[here * SLOTS + g] for g in range(SLOTS)]
    rows = [pl.multiple_of(index_ref[0, here * SLOTS + g] * BW, BW) for g in range(SLOTS)]
    cols = [pl.multiple_of(index_ref[1, here * SLOTS + g] * BW, BW) for g in range(SLOTS)]
    col = lanes((1, BW))
    at = sublanes((BW, BW))
    target = jnp.full((1, BW), -BW, jnp.int32)
    for g in range(SLOTS):
        place = jnp.int32(0)
        for h in range(g):
            place = place + jnp.where((lives[h] == 1) & (owners[h] == owners[g]), 1, 0)
        first = jnp.where(lives[g] == 1, 16 * (2 * owners[g] + place), -BW)
        inside = (col >= 16 * g) & (col < 16 * (g + 1))
        target = jnp.where(inside, first + col - 16 * g, target)
    route_ref[...] = (at == target).astype(F32).astype(BF16)
    target = jnp.full((1, BW), -BW, jnp.int32)
    rank = jnp.int32(0)
    for q in range(OWNERS):
        place = jnp.int32(0)
        firsts = [jnp.int32(-BW)] * 2
        for g in range(SLOTS):
            slot = q * SLOTS + g
            chosen = (mask_ref[slot] == 1) & (owner_ref[slot] == here)
            firsts = [jnp.where(chosen & (place == k), 16 * rank, f) for k, f in enumerate(firsts)]
            place = place + jnp.where(chosen, 1, 0)
            rank = rank + jnp.where(chosen, 1, 0)
        for k in range(2):
            begin = 16 * (2 * q + k)
            inside = (col >= begin) & (col < begin + 16)
            target = jnp.where(inside, firsts[k] + col - begin, target)
    place_ref[...] = (at == target).astype(F32).astype(BF16)
    for c in inactives:
        c.wait()
    for g in range(SLOTS):
        square = lax.dot_general(
            inactive[:, pl.ds(rows[g], BW)],
            inactive[:, pl.ds(cols[g], BW)],
            (((0,), (0,)), ((), ())),
            preferred_element_type=F32,
        )
        density[g] = square.astype(BF16).astype(F32) * lives[g].astype(F32)
    actives[0].wait()
    for g in range(SLOTS):
        column = active[:, pl.ds(cols[g], BW)].astype(F32)
        for p in range(PER):
            wide[pl.ds(ACT * p, ACT), pl.ds(BW * p, BW)] = column
        weights = wide[...].astype(BF16)
        whole[g].wait()
        for k in range(GROUPS):
            joined = jnp.concatenate([blocks[g, k * PER + p] for p in range(PER)], axis=1)
            half = nt(joined, weights)
            halves[pl.ds(g * BW, BW), pl.ds(k * BW, BW)] = half.astype(BF16)
        square = density[g]
        for p in range(ROWS):
            product = blocks[g, p].astype(F32) * square
            part_sum = jnp.sum(product.reshape(BW // 8, 8, BW), axis=0)
            if g == 0:
                sums[p] = part_sum
            else:
                sums[p] = sums[p] + part_sum
    left_side = jnp.concatenate(
        [active[:, pl.ds(rows[g], BW)].astype(F32) * lives[g].astype(F32) for g in range(SLOTS)],
        axis=1,
    ).astype(BF16)
    fitted = jnp.dot(left_side, halves[...], preferred_element_type=F32)
    coupling = jnp.sum(jnp.sum(sums[...], axis=1), axis=1, keepdims=True) * (1.0 / BW)
    coupling = jnp.concatenate([coupling, jnp.zeros((ACT - ROWS, 1), F32)], axis=0)
    high = coupling.astype(BF16).astype(F32)
    low = coupling - high
    spare = lanes((ACT, BW)) >= USED
    for k in range(GROUPS):
        tail = high if k == 0 else low if k == 1 else jnp.zeros_like(high)
        tile = jnp.where(spare, jnp.broadcast_to(tail, (ACT, BW)), fitted[:, k * BW : (k + 1) * BW])
        out_ref[:, pl.ds(k * BW, BW)] = tile.astype(BF16)


def expand_kernel(
    own_ref, one_ref, two_ref, three_ref, blocks, keep_mask, pick_mask, own_out, send_out,
    coupling_ref, spread, left, coulomb, main, rest,
):
    here = lax.axis_index("pair")
    along = lax.axis_index("x")
    total = (own_ref[...].astype(F32) + two_ref[...].astype(F32)) + (
        one_ref[...].astype(F32) + three_ref[...].astype(F32)
    )
    both = total[:, :BW] + total[:, BW : 2 * BW]
    coupling = jnp.sum(jnp.where(lanes((ACT, BW)) == USED, both, 0.0), axis=1, keepdims=True)
    coupling_ref[...] = jnp.broadcast_to(coupling.astype(BF16).astype(F32), (ACT, BW))
    fitted = total.astype(BF16).astype(F32)
    keep = keep_mask[...]
    for t in range(0, ACT, 2):
        pair = jnp.concatenate(
            [jnp.broadcast_to(fitted[t + d : t + d + 1, :], keep.shape) * keep for d in range(2)],
            axis=0,
        )
        spread[pl.ds(t * ACT, 2 * ACT), :] = pair.astype(BF16)
    folded = jnp.dot(
        spread[...], pick_mask[...], preferred_element_type=F32
    ).astype(BF16)
    left[...] = folded
    columns = left[pl.ds(pl.multiple_of(here * BW, BW), BW), :]
    tail = left[pl.ds(4 * BW, PAIRS - 4 * BW), :]
    main[...] = nt(folded, columns)
    rest[...] = nt(folded, jnp.concatenate([tail, tail], axis=0))
    def one(g, carry):
        total_g = jnp.zeros((BW, BW), F32)
        for p in range(ROWS):
            factor = jnp.broadcast_to(coupling_ref[pl.ds(p, 1), :], (BW, BW))
            total_g = total_g + blocks[g, p].astype(F32) * factor
        coulomb[pl.ds(pl.multiple_of(g * BW, BW), BW), :] = total_g
        return carry

    lax.fori_loop(0, SLOTS, one, 0)
    low_lane = lanes((NZ, BW)) < BW // 2
    for step in range(NX):
        x = lax.rem(along + step, NX)
        base = step * NZ * MSG
        for z in range(NZ):
            row = pl.multiple_of(z // 2 * BW + 32 * x + 16 * (z % 2), 16)
            own_out[pl.ds(base + z * MSG, 16), :] = coulomb[pl.ds(row, 16), :]
        for c in range(CORES):
            first = 144 * x + 9 * c
            start = base + 16 + 16 * c
            for s in range(9):
                own_out[pl.ds(start + s, NZ, stride=MSG), :] = main[
                    pl.ds(first + s, NZ, stride=18), :
                ]
            for s in range(7):
                value = rest[pl.ds(first + s, NZ, stride=18), :]
                if s < 2:
                    other = rest[pl.ds(first + 7 + s, NZ, stride=18), :]
                    value = jnp.where(low_lane, value, other)
                own_out[pl.ds(start + 9 + s, NZ, stride=MSG), :] = value
    send_out[...] = own_out[...].astype(BF16)


def along_x_kernel(own_ref, one_ref, two_ref, three_ref, out_ref):
    total = own_ref[...]
    for ref in (one_ref, two_ref, three_ref):
        total = total + ref[...].astype(F32)
    pieces = [total[z * MSG : (z + 1) * MSG] for z in range(NZ)]
    fock = jnp.concatenate([p[0:16] for p in pieces], axis=0).astype(BF16)
    for z in range(NZ):
        out_ref[z, 0:128, :] = fock
        out_ref[z, 128:160, :] = pieces[z][16:MSG].astype(BF16)


def route_kernel(route_ref, parts_ref, out_ref):
    total = jnp.sum(parts_ref[...].astype(F32), axis=0)
    gram = (total[128:160] * (1.0 / AUX)).astype(BF16)
    scaled = total[0:128] * (1.0 / math.sqrt(AUX))
    halves = []
    for h in range(2):
        rows = [scaled[32 * g + 16 * h : 32 * g + 16 * h + 16] for g in range(SLOTS)]
        halves.append(jnp.concatenate(rows + [jnp.zeros((64, BW), F32)], axis=0))
    source = jnp.concatenate(halves, axis=1).astype(BF16)
    chosen = jnp.dot(route_ref[...], source, preferred_element_type=F32).astype(BF16)
    for o in range(OWNERS):
        for x in range(NX):
            for h in range(2):
                out_ref[o * NX + x, 32 * h : 32 * (h + 1), :] = chosen[
                    32 * o : 32 * (o + 1), h * BW : (h + 1) * BW
                ]
            out_ref[o * NX + x, 64:96, :] = gram


def place_kernel(place_ref, own_ref, other_ref, fock_ref, gram_ref):
    core = lax.axis_index("core")
    along = lax.axis_index("x")
    for c, ref in enumerate((other_ref, own_ref)):

        @pl.when(core == c)
        def _(c=c, ref=ref):
            table = place_ref[...]
            for x in range(NX):
                for h in range(2):
                    pieces = jnp.concatenate(
                        [ref[q * NX + x, 32 * h : 32 * (h + 1), :] for q in range(OWNERS)], axis=0
                    )
                    placed = jnp.dot(table, pieces, preferred_element_type=F32)
                    for rank in range(8):
                        row = rank * BW + 32 * x + 16 * h
                        fock_ref[row : row + 16, :] = placed[16 * rank : 16 * (rank + 1)]
            for q in range(OWNERS):
                gram = ref[q * NX + along, 64 + 16 * c : 80 + 16 * c, :].astype(F32)
                gram_ref[:, q * BW : (q + 1) * BW] = gram[0:9]
                if q == 0:
                    gram_ref[0:7, 4 * BW : PAIRS] = gram[9:16, 0 : BW // 2]
                    gram_ref[7:9, 4 * BW : PAIRS] = gram[9:11, BW // 2 : BW]


def from_others(x):
    return [
        lax.ppermute(x, "pair", [(i, (i + s) % OWNERS) for i in range(OWNERS)])
        for s in range(1, OWNERS)
    ]


def from_north(pieces):
    return [
        lax.ppermute(
            pieces[s],
            ("x", "core"),
            [(CORES * i + 1, CORES * ((i + s) % NX) + 1) for i in range(NX)],
        )
        for s in range(1, NX)
    ]


def shards(three_centre, block_mask, block_owner, block_index, active_orbitals, inactive_orbitals):
    dma = pltpu.SemaphoreType.DMA
    inputs = (
        block_mask, block_owner, block_index, three_centre, active_orbitals, inactive_orbitals
    )
    pinned = [pltpu.with_memory_space_constraint(a, pltpu.HBM) for a in inputs]
    message, blocks, routes, places, keep_mask, pick_mask = pl.pallas_call(
        contract_kernel,
        out_shape=[
            pltpu.VMEM((ACT, GROUPS * BW), BF16),
            pltpu.VMEM((SLOTS, ROWS, BW, BW), BF16),
            pltpu.VMEM((BW, BW), BF16),
            pltpu.VMEM((BW, BW), BF16),
            pltpu.VMEM((ACT, GROUPS * BW), F32),
            pltpu.VMEM((GROUPS * BW, BW), BF16),
        ],
        in_specs=[HBM] * 6,
        out_specs=[VMEM] * 6,
        scratch_shapes=[
            pltpu.SMEM((16,), jnp.int32),
            pltpu.SMEM((16,), jnp.int32),
            pltpu.SMEM((2, 16), jnp.int32),
            pltpu.VMEM((ACT, NAO), BF16),
            pltpu.VMEM((NIN, NAO), BF16),
            pltpu.VMEM((BW, PER * BW), F32),
            pltpu.VMEM((SLOTS * BW, GROUPS * BW), BF16),
            pltpu.VMEM((SLOTS, BW, BW), F32),
            pltpu.VMEM((ROWS, 8, BW), F32),
            dma((3,)), dma((SLOTS,)), dma((1,)), dma((SLOTS,)),
        ],
        compiler_params=limit(8192),
        name="contract",
    )(*pinned)
    one, two, three = from_others(message)
    rows = NX * NZ * MSG
    own, send = pl.pallas_call(
        expand_kernel,
        out_shape=[pltpu.VMEM((rows, BW), F32), pltpu.VMEM((rows, BW), BF16)],
        in_specs=[VMEM] * 7,
        out_specs=[VMEM, VMEM],
        scratch_shapes=[
            pltpu.VMEM((ACT, BW), F32),
            pltpu.VMEM((PAIRS, GROUPS * BW), BF16),
            pltpu.VMEM((PAIRS, BW), BF16),
            pltpu.VMEM((SLOTS * BW, BW), F32),
            pltpu.VMEM((PAIRS, BW), F32),
            pltpu.VMEM((PAIRS, BW), F32),
        ],
        compiler_params=limit(8192),
        name="expand",
    )(message, one, two, three, blocks, keep_mask, pick_mask)
    chip_sum = own + lax.ppermute(send, "core", [(0, 1)]).astype(F32)
    chip_sum = chip_sum.reshape(NX, NZ * MSG, BW)
    one, two, three = from_north(chip_sum.astype(BF16))
    pieces = pl.pallas_call(
        along_x_kernel,
        out_shape=pltpu.VMEM((NZ, 160, BW), BF16),
        in_specs=[VMEM] * 4,
        out_specs=VMEM,
        compiler_params=limit(4096),
        name="along_x",
    )(chip_sum[0], one, two, three)
    along_z = lax.all_to_all(pieces, "z", 0, 0, tiled=True)
    pieces = pl.pallas_call(
        route_kernel,
        out_shape=pltpu.VMEM((OWNERS * NX, 96, BW), BF16),
        in_specs=[VMEM] * 2,
        out_specs=VMEM,
        compiler_params=limit(4096),
        name="route",
    )(routes, along_z)
    received = lax.all_to_all(pieces, ("pair", "x"), 0, 0, tiled=True)
    partner = lax.ppermute(received, "core", [(1, 0)])
    fock, integrals = pl.pallas_call(
        place_kernel,
        out_shape=[
            jax.ShapeDtypeStruct((8 * BW, BW), F32),
            jax.ShapeDtypeStruct((9, PAIRS), F32),
        ],
        in_specs=[VMEM] * 3,
        out_specs=[VMEM, VMEM],
        compiler_params=limit(4096),
        name="place",
    )(places, received, partner)
    return (fock.reshape(8, BW, BW), integrals)


def solution(mesh):
    split = Mesh(mesh.devices.reshape(NX, NZ, CORES, OWNERS), ("x", "z", "core", "pair"))
    aux = ("x", "z", "core")
    return jax.shard_map(
        shards,
        mesh=split,
        in_specs=(P("pair", aux, None, None), P(), P(), P(), P(), P()),
        out_specs=(P("pair", None, None), P(aux, None)),
        check_vma=False,
    )
```

```python
import math

import jax
import jax.numpy as jnp
from jax import lax
from jax.experimental import pallas as pl
from jax.experimental.pallas import tpu as pltpu
from jax.sharding import Mesh, PartitionSpec as P

SLOTS = 4
ROWS = 20
BW = 128
ACT = 24
PAIRS = 576
GROUPS = 4
PER = 5
USED = PER * ACT
NX = 4
NZ = 8
CHIPS = NX * NZ
CORES = 2
OWNERS = 4
AUX = 1280
NIN = 256
NAO = 3072
MSG = 24
F32 = jnp.float32
BF16 = jnp.bfloat16

HBM = pl.BlockSpec(memory_space=pltpu.HBM)
VMEM = pl.BlockSpec(memory_space=pltpu.VMEM)


def limit(kib):
    return pltpu.CompilerParams(vmem_limit_bytes=kib << 10)


def nt(a, b):
    return lax.dot_general(a, b, (((1,), (1,)), ((), ())), preferred_element_type=F32)


def lanes(shape):
    return lax.broadcasted_iota(jnp.int32, shape, len(shape) - 1)


def sublanes(shape):
    return lax.broadcasted_iota(jnp.int32, shape, len(shape) - 2)


def contract_kernel(
    mask_hbm, owner_hbm, index_hbm, blocks_hbm, active_hbm, inactive_hbm,
    out_ref, blocks, route_ref, place_ref, keep_mask, pick_mask,
    mask_ref, owner_ref, index_ref, active, inactive, wide, halves, density, sums,
    int_sem, ina_sem, act_sem, block_sem,
):
    here = lax.axis_index("pair")
    ints = [
        pltpu.make_async_copy(index_hbm, index_ref, int_sem.at[0]),
        pltpu.make_async_copy(mask_hbm, mask_ref, int_sem.at[1]),
        pltpu.make_async_copy(owner_hbm, owner_ref, int_sem.at[2]),
    ]
    part = NIN // SLOTS
    inactives = [
        pltpu.make_async_copy(
            inactive_hbm.at[pl.ds(n * part, part)], inactive.at[pl.ds(n * part, part)], ina_sem.at[n]
        )
        for n in range(SLOTS)
    ]
    actives = [pltpu.make_async_copy(active_hbm, active, act_sem.at[0])]
    whole = [
        pltpu.make_async_copy(blocks_hbm.at[g], blocks.at[g], block_sem.at[g]) for g in range(SLOTS)
    ]
    for c in ints + inactives + actives:
        c.start()
    for c in whole:
        c.start(priority=1)
    wide[...] = jnp.zeros_like(wide)
    offset = lanes((ACT, BW)) - sublanes((ACT, BW))
    keep = offset == 0
    for p in range(1, PER):
        keep = keep | (offset == ACT * p)
    keep = jnp.concatenate([keep.astype(F32)] * GROUPS, axis=1)
    keep_mask[...] = keep
    shape = (GROUPS * BW, BW)
    lane = lanes(shape)
    group = (
        (lane >= PER).astype(jnp.int32)
        + (lane >= 2 * PER).astype(jnp.int32)
        + (lane >= 3 * PER).astype(jnp.int32)
    )
    start = group * BW + (lane - group * PER) * ACT
    position = sublanes(shape) - start
    pick = (position >= 0) & (position < ACT) & (lane < ROWS)
    pick_mask[...] = pick.astype(F32).astype(BF16)
    for c in ints:
        c.wait()
    lives = [mask_ref[here * SLOTS + g] for g in range(SLOTS)]
    owners = [owner_ref[here * SLOTS + g] for g in range(SLOTS)]
    rows = [pl.multiple_of(index_ref[0, here * SLOTS + g] * BW, BW) for g in range(SLOTS)]
    cols = [pl.multiple_of(index_ref[1, here * SLOTS + g] * BW, BW) for g in range(SLOTS)]
    col = lanes((1, BW))
    at = sublanes((BW, BW))
    target = jnp.full((1, BW), -BW, jnp.int32)
    for g in range(SLOTS):
        place = jnp.int32(0)
        for h in range(g):
            place = place + jnp.where((lives[h] == 1) & (owners[h] == owners[g]), 1, 0)
        first = jnp.where(lives[g] == 1, 16 * (2 * owners[g] + place), -BW)
        inside = (col >= 16 * g) & (col < 16 * (g + 1))
        target = jnp.where(inside, first + col - 16 * g, target)
    route_ref[...] = (at == target).astype(F32).astype(BF16)
    target = jnp.full((1, BW), -BW, jnp.int32)
    rank = jnp.int32(0)
    for q in range(OWNERS):
        place = jnp.int32(0)
        firsts = [jnp.int32(-BW)] * 2
        for g in range(SLOTS):
            slot = q * SLOTS + g
            chosen = (mask_ref[slot] == 1) & (owner_ref[slot] == here)
            firsts = [jnp.where(chosen & (place == k), 16 * rank, f) for k, f in enumerate(firsts)]
            place = place + jnp.where(chosen, 1, 0)
            rank = rank + jnp.where(chosen, 1, 0)
        for k in range(2):
            begin = 16 * (2 * q + k)
            inside = (col >= begin) & (col < begin + 16)
            target = jnp.where(inside, firsts[k] + col - begin, target)
    place_ref[...] = (at == target).astype(F32).astype(BF16)
    for c in inactives:
        c.wait()
    for g in range(SLOTS):
        square = lax.dot_general(
            inactive[:, pl.ds(rows[g], BW)],
            inactive[:, pl.ds(cols[g], BW)],
            (((0,), (0,)), ((), ())),
            preferred_element_type=F32,
        )
        density[g] = square.astype(BF16).astype(F32) * lives[g].astype(F32)
    actives[0].wait()
    for g in range(SLOTS):
        column = active[:, pl.ds(cols[g], BW)].astype(F32)
        for p in range(PER):
            wide[pl.ds(ACT * p, ACT), pl.ds(BW * p, BW)] = column
        weights = wide[...].astype(BF16)
        whole[g].wait()
        for k in range(GROUPS):
            joined = jnp.concatenate([blocks[g, k * PER + p] for p in range(PER)], axis=1)
            half = nt(joined, weights)
            halves[pl.ds(g * BW, BW), pl.ds(k * BW, BW)] = half.astype(BF16)
        square = density[g]
        for p in range(ROWS):
            product = blocks[g, p].astype(F32) * square
            part_sum = jnp.sum(product.reshape(BW // 8, 8, BW), axis=0)
            if g == 0:
                sums[p] = part_sum
            else:
                sums[p] = sums[p] + part_sum
    left_side = jnp.concatenate(
        [active[:, pl.ds(rows[g], BW)].astype(F32) * lives[g].astype(F32) for g in range(SLOTS)],
        axis=1,
    ).astype(BF16)
    fitted = jnp.dot(left_side, halves[...], preferred_element_type=F32)
    coupling = jnp.sum(jnp.sum(sums[...], axis=1), axis=1, keepdims=True) * (1.0 / BW)
    coupling = jnp.concatenate([coupling, jnp.zeros((ACT - ROWS, 1), F32)], axis=0)
    high = coupling.astype(BF16).astype(F32)
    low = coupling - high
    spare = lanes((ACT, BW)) >= USED
    for k in range(GROUPS):
        tail = high if k == 0 else low if k == 1 else jnp.zeros_like(high)
        tile = jnp.where(spare, jnp.broadcast_to(tail, (ACT, BW)), fitted[:, k * BW : (k + 1) * BW])
        out_ref[:, pl.ds(k * BW, BW)] = tile.astype(BF16)


def expand_kernel(
    own_ref, one_ref, two_ref, three_ref, blocks, keep_mask, pick_mask, keep_ref, send_ref,
    coupling_ref, spread, left, coulomb, main, rest, staged,
):
    here = lax.axis_index("pair")
    core = lax.axis_index("core")
    along = lax.axis_index("x")
    total = (own_ref[...].astype(F32) + two_ref[...].astype(F32)) + (
        one_ref[...].astype(F32) + three_ref[...].astype(F32)
    )
    both = total[:, :BW] + total[:, BW : 2 * BW]
    coupling = jnp.sum(jnp.where(lanes((ACT, BW)) == USED, both, 0.0), axis=1, keepdims=True)
    coupling_ref[...] = jnp.broadcast_to(coupling.astype(BF16).astype(F32), (ACT, BW))
    fitted = total.astype(BF16).astype(F32)
    keep = keep_mask[...]
    for t in range(0, ACT, 2):
        pair = jnp.concatenate(
            [jnp.broadcast_to(fitted[t + d : t + d + 1, :], keep.shape) * keep for d in range(2)],
            axis=0,
        )
        spread[pl.ds(t * ACT, 2 * ACT), :] = pair.astype(BF16)
    folded = jnp.dot(
        spread[...], pick_mask[...], preferred_element_type=F32
    ).astype(BF16)
    left[...] = folded
    columns = left[pl.ds(pl.multiple_of(here * BW, BW), BW), :]
    tail = left[pl.ds(4 * BW, PAIRS - 4 * BW), :]
    main[...] = nt(folded, columns)
    rest[...] = nt(folded, jnp.concatenate([tail, tail], axis=0))
    def one(g, carry):
        total_g = jnp.zeros((BW, BW), F32)
        for p in range(ROWS):
            factor = jnp.broadcast_to(coupling_ref[pl.ds(p, 1), :], (BW, BW))
            total_g = total_g + blocks[g, p].astype(F32) * factor
        coulomb[pl.ds(pl.multiple_of(g * BW, BW), BW), :] = total_g
        return carry

    lax.fori_loop(0, SLOTS, one, 0)
    low_lane = lanes((NZ, BW)) < BW // 2
    for ref, which in ((staged, 1 - core), (keep_ref, core)):
        for step in range(NX):
            x = lax.rem(along + step, NX)
            base = step * NZ * MSG
            for z in range(NZ):
                row = pl.multiple_of(z // 2 * BW + 32 * x + 16 * which + 8 * (z % 2), 8)
                ref[pl.ds(base + z * MSG, 8), :] = coulomb[pl.ds(row, 8), :]
            first = 144 * x + 9 * which
            for s in range(9):
                ref[pl.ds(base + 8 + s, NZ, stride=MSG), :] = main[pl.ds(first + s, NZ, stride=18), :]
            for s in range(7):
                value = rest[pl.ds(first + s, NZ, stride=18), :]
                if s < 2:
                    other = rest[pl.ds(first + 7 + s, NZ, stride=18), :]
                    value = jnp.where(low_lane, value, other)
                ref[pl.ds(base + 17 + s, NZ, stride=MSG), :] = value
    send_ref[...] = staged[...].astype(BF16)


def along_x_kernel(own_ref, one_ref, two_ref, three_ref, out_ref):
    total = own_ref[...]
    for ref in (one_ref, two_ref, three_ref):
        total = total + ref[...].astype(F32)
    pieces = [total[z * MSG : (z + 1) * MSG] for z in range(NZ)]
    fock = jnp.concatenate([p[0:8] for p in pieces], axis=0).astype(BF16)
    for z in range(NZ):
        out_ref[z, 0:64, :] = fock
        out_ref[z, 64:80, :] = pieces[z][8:MSG].astype(BF16)


def route_kernel(route_ref, parts_ref, out_ref):
    total = jnp.sum(parts_ref[...].astype(F32), axis=0)
    gram = (total[64:80] * (1.0 / AUX)).astype(BF16)
    scaled = total[0:64] * (1.0 / math.sqrt(AUX))
    scaled = jnp.concatenate([scaled, jnp.zeros_like(scaled)], axis=0).astype(BF16)
    chosen = jnp.dot(route_ref[...], scaled, preferred_element_type=F32).astype(BF16)
    for o in range(OWNERS):
        for x in range(NX):
            out_ref[o * NX + x, 0:32, :] = chosen[32 * o : 32 * (o + 1)]
            out_ref[o * NX + x, 32:48, :] = gram


def place_kernel(place_ref, own_ref, other_ref, fock_ref, gram_ref):
    core = lax.axis_index("core")
    along = lax.axis_index("x")
    table = place_ref[...]
    for n, ref in enumerate((own_ref, other_ref)):
        which = core if n == 0 else 1 - core
        for x in range(NX):
            pieces = jnp.concatenate([ref[q * NX + x, 0:32, :] for q in range(OWNERS)], axis=0)
            placed = jnp.dot(table, pieces, preferred_element_type=F32)
            for rank in range(8):
                row = pl.multiple_of(rank * BW + 32 * x + 16 * which, 16)
                fock_ref[pl.ds(row, 16), :] = placed[16 * rank : 16 * (rank + 1)]
    for q in range(OWNERS):
        gram = own_ref[q * NX + along, 32:48, :].astype(F32)
        gram_ref[:, q * BW : (q + 1) * BW] = gram[0:9]
        if q == 0:
            gram_ref[0:7, 4 * BW : PAIRS] = gram[9:16, 0 : BW // 2]
            gram_ref[7:9, 4 * BW : PAIRS] = gram[9:11, BW // 2 : BW]


def from_others(x, axis="pair"):
    return [
        lax.ppermute(x if axis == "pair" else x[s], axis, [(i, (i + s) % 4) for i in range(4)])
        for s in range(1, 4)
    ]


def shards(three_centre, block_mask, block_owner, block_index, active_orbitals, inactive_orbitals):
    dma = pltpu.SemaphoreType.DMA
    inputs = (
        block_mask, block_owner, block_index, three_centre, active_orbitals, inactive_orbitals
    )
    pinned = [pltpu.with_memory_space_constraint(a, pltpu.HBM) for a in inputs]
    message, blocks, routes, places, keep_mask, pick_mask = pl.pallas_call(
        contract_kernel,
        out_shape=[
            pltpu.VMEM((ACT, GROUPS * BW), BF16),
            pltpu.VMEM((SLOTS, ROWS, BW, BW), BF16),
            pltpu.VMEM((BW, BW), BF16),
            pltpu.VMEM((BW, BW), BF16),
            pltpu.VMEM((ACT, GROUPS * BW), F32),
            pltpu.VMEM((GROUPS * BW, BW), BF16),
        ],
        in_specs=[HBM] * 6,
        out_specs=[VMEM] * 6,
        scratch_shapes=[
            pltpu.SMEM((16,), jnp.int32),
            pltpu.SMEM((16,), jnp.int32),
            pltpu.SMEM((2, 16), jnp.int32),
            pltpu.VMEM((ACT, NAO), BF16),
            pltpu.VMEM((NIN, NAO), BF16),
            pltpu.VMEM((BW, PER * BW), F32),
            pltpu.VMEM((SLOTS * BW, GROUPS * BW), BF16),
            pltpu.VMEM((SLOTS, BW, BW), F32),
            pltpu.VMEM((ROWS, 8, BW), F32),
            dma((3,)), dma((SLOTS,)), dma((1,)), dma((SLOTS,)),
        ],
        compiler_params=limit(8192),
        name="contract",
    )(*pinned)
    one, two, three = from_others(message)
    rows = CHIPS * MSG
    keep, send = pl.pallas_call(
        expand_kernel,
        out_shape=[pltpu.VMEM((rows, BW), F32), pltpu.VMEM((rows, BW), BF16)],
        in_specs=[VMEM] * 7,
        out_specs=[VMEM, VMEM],
        scratch_shapes=[
            pltpu.VMEM((ACT, BW), F32),
            pltpu.VMEM((PAIRS, GROUPS * BW), BF16),
            pltpu.VMEM((PAIRS, BW), BF16),
            pltpu.VMEM((SLOTS * BW, BW), F32),
            pltpu.VMEM((PAIRS, BW), F32),
            pltpu.VMEM((PAIRS, BW), F32),
            pltpu.VMEM((rows, BW), F32),
        ],
        compiler_params=limit(8192),
        name="expand",
    )(message, one, two, three, blocks, keep_mask, pick_mask)
    swap = [(0, 1), (1, 0)]
    chip_sum = (keep + lax.ppermute(send, "core", swap).astype(F32)).reshape(NX, NZ * MSG, BW)
    one, two, three = from_others(chip_sum.astype(BF16), "x")
    pieces = pl.pallas_call(
        along_x_kernel,
        out_shape=pltpu.VMEM((NZ, 80, BW), BF16),
        in_specs=[VMEM] * 4,
        out_specs=VMEM,
        compiler_params=limit(4096),
        name="along_x",
    )(chip_sum[0], one, two, three)
    along_z = lax.all_to_all(pieces, "z", 0, 0, tiled=True)
    pieces = pl.pallas_call(
        route_kernel,
        out_shape=pltpu.VMEM((OWNERS * NX, 48, BW), BF16),
        in_specs=[VMEM] * 2,
        out_specs=VMEM,
        compiler_params=limit(4096),
        name="route",
    )(routes, along_z)
    received = lax.all_to_all(pieces, ("pair", "x"), 0, 0, tiled=True)
    partner = lax.ppermute(received, "core", swap)
    fock, integrals = pl.pallas_call(
        place_kernel,
        out_shape=[
            jax.ShapeDtypeStruct((8 * BW, BW), F32),
            jax.ShapeDtypeStruct((9, PAIRS), F32),
        ],
        in_specs=[VMEM] * 3,
        out_specs=[VMEM, VMEM],
        compiler_params=limit(4096),
        name="place",
    )(places, received, partner)
    return (fock.reshape(8, BW, BW), integrals)


def solution(mesh):
    split = Mesh(mesh.devices.reshape(NX, NZ, CORES, OWNERS), ("x", "z", "core", "pair"))
    aux = ("x", "z", "core")
    return jax.shard_map(
        shards,
        mesh=split,
        in_specs=(P("pair", aux, None, None), P(), P(), P(), P(), P()),
        out_specs=(P("pair", None, None), P(aux, None)),
        check_vma=False,
    )
```

```python
import math

import jax
import jax.numpy as jnp
from jax import lax
from jax.experimental import pallas as pl
from jax.experimental.pallas import tpu as pltpu
from jax.sharding import Mesh, PartitionSpec as P

SLOTS = 4
ROWS = 20
BW = 128
ACT = 24
PAIRS = 576
GROUPS = 4
PER = 5
USED = PER * ACT
NX = 4
NZ = 8
CHIPS = NX * NZ
CORES = 2
OWNERS = 4
AUX = 1280
NIN = 256
NAO = 3072
MSG = 24
F32 = jnp.float32
BF16 = jnp.bfloat16

HBM = pl.BlockSpec(memory_space=pltpu.HBM)
VMEM = pl.BlockSpec(memory_space=pltpu.VMEM)


def limit(kib):
    return pltpu.CompilerParams(vmem_limit_bytes=kib << 10)


def nt(a, b):
    return lax.dot_general(a, b, (((1,), (1,)), ((), ())), preferred_element_type=F32)


def half_here():
    z = lax.axis_index("z")
    x = lax.axis_index("x")
    flips = jnp.where(z >= NZ // 2, 1, 0) + jnp.where(x >= NX // 2, 1, 0)
    return lax.rem(lax.axis_index("core") + flips, CORES)


def flip_x(x):
    return x // (NX // 2)


def flip_z(z):
    return z // (NZ // 2)


Z_GROUPS = [[z * CORES + (g + flip_z(z)) % CORES for z in range(NZ)] for g in range(CORES)]
X_GROUPS = [
    [(q * NX + x) * CORES + (g + flip_x(x)) % CORES for q in range(OWNERS) for x in range(NX)]
    for g in range(CORES)
]


def lanes(shape):
    return lax.broadcasted_iota(jnp.int32, shape, len(shape) - 1)


def sublanes(shape):
    return lax.broadcasted_iota(jnp.int32, shape, len(shape) - 2)


def contract_kernel(
    mask_hbm, owner_hbm, index_hbm, blocks_hbm, active_hbm, inactive_hbm,
    out_ref, blocks, route_ref, place_ref, keep_mask, pick_mask,
    mask_ref, owner_ref, index_ref, active, inactive, wide, halves, density, sums,
    int_sem, ina_sem, act_sem, block_sem,
):
    here = lax.axis_index("pair")
    ints = [
        pltpu.make_async_copy(index_hbm, index_ref, int_sem.at[0]),
        pltpu.make_async_copy(mask_hbm, mask_ref, int_sem.at[1]),
        pltpu.make_async_copy(owner_hbm, owner_ref, int_sem.at[2]),
    ]
    part = NIN // SLOTS
    inactives = [
        pltpu.make_async_copy(
            inactive_hbm.at[pl.ds(n * part, part)], inactive.at[pl.ds(n * part, part)], ina_sem.at[n]
        )
        for n in range(SLOTS)
    ]
    actives = [pltpu.make_async_copy(active_hbm, active, act_sem.at[0])]
    whole = [
        pltpu.make_async_copy(blocks_hbm.at[g], blocks.at[g], block_sem.at[g]) for g in range(SLOTS)
    ]
    for c in ints + inactives + actives:
        c.start()
    for c in whole:
        c.start(priority=1)
    wide[...] = jnp.zeros_like(wide)
    offset = lanes((ACT, BW)) - sublanes((ACT, BW))
    keep = offset == 0
    for p in range(1, PER):
        keep = keep | (offset == ACT * p)
    keep = jnp.concatenate([keep.astype(F32)] * GROUPS, axis=1)
    keep_mask[...] = keep
    shape = (GROUPS * BW, BW)
    lane = lanes(shape)
    group = (
        (lane >= PER).astype(jnp.int32)
        + (lane >= 2 * PER).astype(jnp.int32)
        + (lane >= 3 * PER).astype(jnp.int32)
    )
    start = group * BW + (lane - group * PER) * ACT
    position = sublanes(shape) - start
    pick = (position >= 0) & (position < ACT) & (lane < ROWS)
    pick_mask[...] = pick.astype(F32).astype(BF16)
    for c in ints:
        c.wait()
    lives = [mask_ref[here * SLOTS + g] for g in range(SLOTS)]
    owners = [owner_ref[here * SLOTS + g] for g in range(SLOTS)]
    rows = [pl.multiple_of(index_ref[0, here * SLOTS + g] * BW, BW) for g in range(SLOTS)]
    cols = [pl.multiple_of(index_ref[1, here * SLOTS + g] * BW, BW) for g in range(SLOTS)]
    col = lanes((1, BW))
    at = sublanes((BW, BW))
    target = jnp.full((1, BW), -BW, jnp.int32)
    for g in range(SLOTS):
        place = jnp.int32(0)
        for h in range(g):
            place = place + jnp.where((lives[h] == 1) & (owners[h] == owners[g]), 1, 0)
        first = jnp.where(lives[g] == 1, 16 * (2 * owners[g] + place), -BW)
        inside = (col >= 16 * g) & (col < 16 * (g + 1))
        target = jnp.where(inside, first + col - 16 * g, target)
    route_ref[...] = (at == target).astype(F32).astype(BF16)
    target = jnp.full((1, BW), -BW, jnp.int32)
    rank = jnp.int32(0)
    for q in range(OWNERS):
        place = jnp.int32(0)
        firsts = [jnp.int32(-BW)] * 2
        for g in range(SLOTS):
            slot = q * SLOTS + g
            chosen = (mask_ref[slot] == 1) & (owner_ref[slot] == here)
            firsts = [jnp.where(chosen & (place == k), 16 * rank, f) for k, f in enumerate(firsts)]
            place = place + jnp.where(chosen, 1, 0)
            rank = rank + jnp.where(chosen, 1, 0)
        for k in range(2):
            begin = 16 * (2 * q + k)
            inside = (col >= begin) & (col < begin + 16)
            target = jnp.where(inside, firsts[k] + col - begin, target)
    place_ref[...] = (at == target).astype(F32).astype(BF16)
    for c in inactives:
        c.wait()
    for g in range(SLOTS):
        square = lax.dot_general(
            inactive[:, pl.ds(rows[g], BW)],
            inactive[:, pl.ds(cols[g], BW)],
            (((0,), (0,)), ((), ())),
            preferred_element_type=F32,
        )
        density[g] = square.astype(BF16).astype(F32) * lives[g].astype(F32)
    actives[0].wait()
    for g in range(SLOTS):
        column = active[:, pl.ds(cols[g], BW)].astype(F32)
        for p in range(PER):
            wide[pl.ds(ACT * p, ACT), pl.ds(BW * p, BW)] = column
        weights = wide[...].astype(BF16)
        whole[g].wait()
        for k in range(GROUPS):
            joined = jnp.concatenate([blocks[g, k * PER + p] for p in range(PER)], axis=1)
            half = nt(joined, weights)
            halves[pl.ds(g * BW, BW), pl.ds(k * BW, BW)] = half.astype(BF16)
        square = density[g]
        for p in range(ROWS):
            product = blocks[g, p].astype(F32) * square
            part_sum = jnp.sum(product.reshape(BW // 8, 8, BW), axis=0)
            if g == 0:
                sums[p] = part_sum
            else:
                sums[p] = sums[p] + part_sum
    left_side = jnp.concatenate(
        [active[:, pl.ds(rows[g], BW)].astype(F32) * lives[g].astype(F32) for g in range(SLOTS)],
        axis=1,
    ).astype(BF16)
    fitted = jnp.dot(left_side, halves[...], preferred_element_type=F32)
    coupling = jnp.sum(jnp.sum(sums[...], axis=1), axis=1, keepdims=True) * (1.0 / BW)
    coupling = jnp.concatenate([coupling, jnp.zeros((ACT - ROWS, 1), F32)], axis=0)
    high = coupling.astype(BF16).astype(F32)
    low = coupling - high
    spare = lanes((ACT, BW)) >= USED
    for k in range(GROUPS):
        tail = high if k == 0 else low if k == 1 else jnp.zeros_like(high)
        tile = jnp.where(spare, jnp.broadcast_to(tail, (ACT, BW)), fitted[:, k * BW : (k + 1) * BW])
        out_ref[:, pl.ds(k * BW, BW)] = tile.astype(BF16)


def expand_kernel(
    own_ref, one_ref, two_ref, three_ref, blocks, keep_mask, pick_mask, keep_ref, send_ref,
    coupling_ref, spread, left, coulomb, main, rest, staged,
):
    here = lax.axis_index("pair")
    core = half_here()
    along = lax.axis_index("x")
    total = (own_ref[...].astype(F32) + two_ref[...].astype(F32)) + (
        one_ref[...].astype(F32) + three_ref[...].astype(F32)
    )
    both = total[:, :BW] + total[:, BW : 2 * BW]
    coupling = jnp.sum(jnp.where(lanes((ACT, BW)) == USED, both, 0.0), axis=1, keepdims=True)
    coupling_ref[...] = jnp.broadcast_to(coupling.astype(BF16).astype(F32), (ACT, BW))
    fitted = total.astype(BF16).astype(F32)
    keep = keep_mask[...]
    for t in range(0, ACT, 2):
        pair = jnp.concatenate(
            [jnp.broadcast_to(fitted[t + d : t + d + 1, :], keep.shape) * keep for d in range(2)],
            axis=0,
        )
        spread[pl.ds(t * ACT, 2 * ACT), :] = pair.astype(BF16)
    folded = jnp.dot(
        spread[...], pick_mask[...], preferred_element_type=F32
    ).astype(BF16)
    left[...] = folded
    columns = left[pl.ds(pl.multiple_of(here * BW, BW), BW), :]
    tail = left[pl.ds(4 * BW, PAIRS - 4 * BW), :]
    main[...] = nt(folded, columns)
    rest[...] = nt(folded, jnp.concatenate([tail, tail], axis=0))
    def one(g, carry):
        total_g = jnp.zeros((BW, BW), F32)
        for p in range(ROWS):
            factor = jnp.broadcast_to(coupling_ref[pl.ds(p, 1), :], (BW, BW))
            total_g = total_g + blocks[g, p].astype(F32) * factor
        coulomb[pl.ds(pl.multiple_of(g * BW, BW), BW), :] = total_g
        return carry

    lax.fori_loop(0, SLOTS, one, 0)
    low_lane = lanes((NZ, BW)) < BW // 2
    for ref, which in ((staged, 1 - core), (keep_ref, core)):
        for step in range(NX):
            x = lax.rem(along + step, NX)
            base = step * NZ * MSG
            for z in range(NZ):
                row = pl.multiple_of(z // 2 * BW + 32 * x + 16 * which + 8 * (z % 2), 8)
                ref[pl.ds(base + z * MSG, 8), :] = coulomb[pl.ds(row, 8), :]
            first = 144 * x + 9 * which
            for s in range(9):
                ref[pl.ds(base + 8 + s, NZ, stride=MSG), :] = main[pl.ds(first + s, NZ, stride=18), :]
            for s in range(7):
                value = rest[pl.ds(first + s, NZ, stride=18), :]
                if s < 2:
                    other = rest[pl.ds(first + 7 + s, NZ, stride=18), :]
                    value = jnp.where(low_lane, value, other)
                ref[pl.ds(base + 17 + s, NZ, stride=MSG), :] = value
    send_ref[...] = staged[...].astype(BF16)


def along_x_kernel(own_ref, one_ref, two_ref, three_ref, out_ref):
    total = own_ref[...]
    for ref in (one_ref, two_ref, three_ref):
        total = total + ref[...].astype(F32)
    pieces = [total[z * MSG : (z + 1) * MSG] for z in range(NZ)]
    fock = jnp.concatenate([p[0:8] for p in pieces], axis=0).astype(BF16)
    for z in range(NZ):
        out_ref[z, 0:64, :] = fock
        out_ref[z, 64:80, :] = pieces[z][8:MSG].astype(BF16)


def route_kernel(route_ref, parts_ref, out_ref):
    total = jnp.sum(parts_ref[...].astype(F32), axis=0)
    gram = (total[64:80] * (1.0 / AUX)).astype(BF16)
    scaled = total[0:64] * (1.0 / math.sqrt(AUX))
    scaled = jnp.concatenate([scaled, jnp.zeros_like(scaled)], axis=0).astype(BF16)
    chosen = jnp.dot(route_ref[...], scaled, preferred_element_type=F32).astype(BF16)
    for o in range(OWNERS):
        for x in range(NX):
            out_ref[o * NX + x, 0:32, :] = chosen[32 * o : 32 * (o + 1)]
            out_ref[o * NX + x, 32:48, :] = gram


def place_kernel(place_ref, own_ref, other_ref, fock_ref, gram_ref):
    core = lax.axis_index("core")
    held = half_here()
    along = lax.axis_index("x")
    table = place_ref[...]
    for n, ref in enumerate((own_ref, other_ref)):
        which = held if n == 0 else 1 - held
        for x in range(NX):
            pieces = jnp.concatenate([ref[q * NX + x, 0:32, :] for q in range(OWNERS)], axis=0)
            placed = jnp.dot(table, pieces, preferred_element_type=F32)
            for rank in range(8):
                row = pl.multiple_of(rank * BW + 32 * x + 16 * which, 16)
                fock_ref[pl.ds(row, 16), :] = placed[16 * rank : 16 * (rank + 1)]
    for same, ref in ((True, own_ref), (False, other_ref)):

        @pl.when((held == core) == same)
        def _(ref=ref):
            for q in range(OWNERS):
                gram = ref[q * NX + along, 32:48, :].astype(F32)
                gram_ref[:, q * BW : (q + 1) * BW] = gram[0:9]
                if q == 0:
                    gram_ref[0:7, 4 * BW : PAIRS] = gram[9:16, 0 : BW // 2]
                    gram_ref[7:9, 4 * BW : PAIRS] = gram[9:11, BW // 2 : BW]


def from_others(x):
    return [
        lax.ppermute(x, "pair", [(i, (i + s) % OWNERS) for i in range(OWNERS)])
        for s in range(1, OWNERS)
    ]


def along(pieces):
    moved = []
    for s in range(1, NX):
        pairs = []
        for x in range(NX):
            to = (x + s) % NX
            for c in range(CORES):
                pairs.append((x * CORES + c, to * CORES + (c + flip_x(x) + flip_x(to)) % CORES))
        moved.append(lax.ppermute(pieces[s], ("x", "core"), pairs))
    return moved


def shards(three_centre, block_mask, block_owner, block_index, active_orbitals, inactive_orbitals):
    dma = pltpu.SemaphoreType.DMA
    inputs = (
        block_mask, block_owner, block_index, three_centre, active_orbitals, inactive_orbitals
    )
    pinned = [pltpu.with_memory_space_constraint(a, pltpu.HBM) for a in inputs]
    message, blocks, routes, places, keep_mask, pick_mask = pl.pallas_call(
        contract_kernel,
        out_shape=[
            pltpu.VMEM((ACT, GROUPS * BW), BF16),
            pltpu.VMEM((SLOTS, ROWS, BW, BW), BF16),
            pltpu.VMEM((BW, BW), BF16),
            pltpu.VMEM((BW, BW), BF16),
            pltpu.VMEM((ACT, GROUPS * BW), F32),
            pltpu.VMEM((GROUPS * BW, BW), BF16),
        ],
        in_specs=[HBM] * 6,
        out_specs=[VMEM] * 6,
        scratch_shapes=[
            pltpu.SMEM((16,), jnp.int32),
            pltpu.SMEM((16,), jnp.int32),
            pltpu.SMEM((2, 16), jnp.int32),
            pltpu.VMEM((ACT, NAO), BF16),
            pltpu.VMEM((NIN, NAO), BF16),
            pltpu.VMEM((BW, PER * BW), F32),
            pltpu.VMEM((SLOTS * BW, GROUPS * BW), BF16),
            pltpu.VMEM((SLOTS, BW, BW), F32),
            pltpu.VMEM((ROWS, 8, BW), F32),
            dma((3,)), dma((SLOTS,)), dma((1,)), dma((SLOTS,)),
        ],
        compiler_params=limit(8192),
        name="contract",
    )(*pinned)
    one, two, three = from_others(message)
    rows = CHIPS * MSG
    keep, send = pl.pallas_call(
        expand_kernel,
        out_shape=[pltpu.VMEM((rows, BW), F32), pltpu.VMEM((rows, BW), BF16)],
        in_specs=[VMEM] * 7,
        out_specs=[VMEM, VMEM],
        scratch_shapes=[
            pltpu.VMEM((ACT, BW), F32),
            pltpu.VMEM((PAIRS, GROUPS * BW), BF16),
            pltpu.VMEM((PAIRS, BW), BF16),
            pltpu.VMEM((SLOTS * BW, BW), F32),
            pltpu.VMEM((PAIRS, BW), F32),
            pltpu.VMEM((PAIRS, BW), F32),
            pltpu.VMEM((rows, BW), F32),
        ],
        compiler_params=limit(8192),
        name="expand",
    )(message, one, two, three, blocks, keep_mask, pick_mask)
    swap = [(0, 1), (1, 0)]
    chip_sum = (keep + lax.ppermute(send, "core", swap).astype(F32)).reshape(NX, NZ * MSG, BW)
    one, two, three = along(chip_sum.astype(BF16))
    pieces = pl.pallas_call(
        along_x_kernel,
        out_shape=pltpu.VMEM((NZ, 80, BW), BF16),
        in_specs=[VMEM] * 4,
        out_specs=VMEM,
        compiler_params=limit(4096),
        name="along_x",
    )(chip_sum[0], one, two, three)
    along_z = lax.all_to_all(
        pieces, ("z", "core"), 0, 0, tiled=True, axis_index_groups=Z_GROUPS
    )
    pieces = pl.pallas_call(
        route_kernel,
        out_shape=pltpu.VMEM((OWNERS * NX, 48, BW), BF16),
        in_specs=[VMEM] * 2,
        out_specs=VMEM,
        compiler_params=limit(4096),
        name="route",
    )(routes, along_z)
    received = lax.all_to_all(
        pieces, ("pair", "x", "core"), 0, 0, tiled=True, axis_index_groups=X_GROUPS
    )
    partner = lax.ppermute(received, "core", swap)
    fock, integrals = pl.pallas_call(
        place_kernel,
        out_shape=[
            jax.ShapeDtypeStruct((8 * BW, BW), F32),
            jax.ShapeDtypeStruct((9, PAIRS), F32),
        ],
        in_specs=[VMEM] * 3,
        out_specs=[VMEM, VMEM],
        compiler_params=limit(4096),
        name="place",
    )(places, received, partner)
    return (fock.reshape(8, BW, BW), integrals)


def solution(mesh):
    split = Mesh(mesh.devices.reshape(NX, NZ, CORES, OWNERS), ("x", "z", "core", "pair"))
    aux = ("x", "z", "core")
    return jax.shard_map(
        shards,
        mesh=split,
        in_specs=(P("pair", aux, None, None), P(), P(), P(), P(), P()),
        out_specs=(P("pair", None, None), P(aux, None)),
        check_vma=False,
    )
```

```python
import math

import jax
import jax.numpy as jnp
from jax import lax
from jax.experimental import pallas as pl
from jax.experimental.pallas import tpu as pltpu
from jax.sharding import Mesh, PartitionSpec as P

SLOTS = 4
ROWS = 20
BW = 128
ACT = 24
PAIRS = 576
GROUPS = 4
PER = 5
USED = PER * ACT
NX = 4
NZ = 8
CHIPS = NX * NZ
CORES = 2
OWNERS = 4
AUX = 1280
NIN = 256
NAO = 3072
MSG = 24
F32 = jnp.float32
BF16 = jnp.bfloat16

HBM = pl.BlockSpec(memory_space=pltpu.HBM)
VMEM = pl.BlockSpec(memory_space=pltpu.VMEM)


def limit(kib):
    return pltpu.CompilerParams(vmem_limit_bytes=kib << 10)


def nt(a, b):
    return lax.dot_general(a, b, (((1,), (1,)), ((), ())), preferred_element_type=F32)


def half_here():
    flips = jnp.where(lax.axis_index("x") >= NX // 2, 1, 0)
    return lax.rem(lax.axis_index("core") + flips, CORES)


def flip_x(x):
    return x // (NX // 2)


X_GROUPS = [
    [(q * NX + x) * CORES + (g + flip_x(x)) % CORES for q in range(OWNERS) for x in range(NX)]
    for g in range(CORES)
]


def lanes(shape):
    return lax.broadcasted_iota(jnp.int32, shape, len(shape) - 1)


def sublanes(shape):
    return lax.broadcasted_iota(jnp.int32, shape, len(shape) - 2)


def contract_kernel(
    mask_hbm, owner_hbm, index_hbm, blocks_hbm, active_hbm, inactive_hbm,
    out_ref, blocks, route_ref, place_ref, keep_mask, pick_mask,
    mask_ref, owner_ref, index_ref, active, inactive, wide, halves, density, sums,
    int_sem, ina_sem, act_sem, block_sem,
):
    here = lax.axis_index("pair")
    ints = [
        pltpu.make_async_copy(index_hbm, index_ref, int_sem.at[0]),
        pltpu.make_async_copy(mask_hbm, mask_ref, int_sem.at[1]),
        pltpu.make_async_copy(owner_hbm, owner_ref, int_sem.at[2]),
    ]
    part = NIN // SLOTS
    inactives = [
        pltpu.make_async_copy(
            inactive_hbm.at[pl.ds(n * part, part)], inactive.at[pl.ds(n * part, part)], ina_sem.at[n]
        )
        for n in range(SLOTS)
    ]
    actives = [pltpu.make_async_copy(active_hbm, active, act_sem.at[0])]
    whole = [
        pltpu.make_async_copy(blocks_hbm.at[g], blocks.at[g], block_sem.at[g]) for g in range(SLOTS)
    ]
    for c in ints + inactives + actives:
        c.start()
    for c in whole:
        c.start(priority=1)
    wide[...] = jnp.zeros_like(wide)
    offset = lanes((ACT, BW)) - sublanes((ACT, BW))
    keep = offset == 0
    for p in range(1, PER):
        keep = keep | (offset == ACT * p)
    keep = jnp.concatenate([keep.astype(F32)] * GROUPS, axis=1)
    keep_mask[...] = keep
    shape = (GROUPS * BW, BW)
    lane = lanes(shape)
    group = (
        (lane >= PER).astype(jnp.int32)
        + (lane >= 2 * PER).astype(jnp.int32)
        + (lane >= 3 * PER).astype(jnp.int32)
    )
    start = group * BW + (lane - group * PER) * ACT
    position = sublanes(shape) - start
    pick = (position >= 0) & (position < ACT) & (lane < ROWS)
    pick_mask[...] = pick.astype(F32).astype(BF16)
    for c in ints:
        c.wait()
    lives = [mask_ref[here * SLOTS + g] for g in range(SLOTS)]
    owners = [owner_ref[here * SLOTS + g] for g in range(SLOTS)]
    rows = [pl.multiple_of(index_ref[0, here * SLOTS + g] * BW, BW) for g in range(SLOTS)]
    cols = [pl.multiple_of(index_ref[1, here * SLOTS + g] * BW, BW) for g in range(SLOTS)]
    col = lanes((1, BW))
    at = sublanes((BW, BW))
    target = jnp.full((1, BW), -BW, jnp.int32)
    for g in range(SLOTS):
        place = jnp.int32(0)
        for h in range(g):
            place = place + jnp.where((lives[h] == 1) & (owners[h] == owners[g]), 1, 0)
        first = jnp.where(lives[g] == 1, 16 * (2 * owners[g] + place), -BW)
        inside = (col >= 16 * g) & (col < 16 * (g + 1))
        target = jnp.where(inside, first + col - 16 * g, target)
    route_ref[...] = (at == target).astype(F32).astype(BF16)
    target = jnp.full((1, BW), -BW, jnp.int32)
    rank = jnp.int32(0)
    for q in range(OWNERS):
        place = jnp.int32(0)
        firsts = [jnp.int32(-BW)] * 2
        for g in range(SLOTS):
            slot = q * SLOTS + g
            chosen = (mask_ref[slot] == 1) & (owner_ref[slot] == here)
            firsts = [jnp.where(chosen & (place == k), 16 * rank, f) for k, f in enumerate(firsts)]
            place = place + jnp.where(chosen, 1, 0)
            rank = rank + jnp.where(chosen, 1, 0)
        for k in range(2):
            begin = 16 * (2 * q + k)
            inside = (col >= begin) & (col < begin + 16)
            target = jnp.where(inside, firsts[k] + col - begin, target)
    place_ref[...] = (at == target).astype(F32).astype(BF16)
    for c in inactives:
        c.wait()
    for g in range(SLOTS):
        square = lax.dot_general(
            inactive[:, pl.ds(rows[g], BW)],
            inactive[:, pl.ds(cols[g], BW)],
            (((0,), (0,)), ((), ())),
            preferred_element_type=F32,
        )
        density[g] = square.astype(BF16).astype(F32) * lives[g].astype(F32)
    actives[0].wait()
    for g in range(SLOTS):
        column = active[:, pl.ds(cols[g], BW)].astype(F32)
        for p in range(PER):
            wide[pl.ds(ACT * p, ACT), pl.ds(BW * p, BW)] = column
        weights = wide[...].astype(BF16)
        whole[g].wait()
        for k in range(GROUPS):
            joined = jnp.concatenate([blocks[g, k * PER + p] for p in range(PER)], axis=1)
            half = nt(joined, weights)
            halves[pl.ds(g * BW, BW), pl.ds(k * BW, BW)] = half.astype(BF16)
        square = density[g]
        for p in range(ROWS):
            product = blocks[g, p].astype(F32) * square
            part_sum = jnp.sum(product.reshape(BW // 8, 8, BW), axis=0)
            if g == 0:
                sums[p] = part_sum
            else:
                sums[p] = sums[p] + part_sum
    left_side = jnp.concatenate(
        [active[:, pl.ds(rows[g], BW)].astype(F32) * lives[g].astype(F32) for g in range(SLOTS)],
        axis=1,
    ).astype(BF16)
    fitted = jnp.dot(left_side, halves[...], preferred_element_type=F32)
    coupling = jnp.sum(jnp.sum(sums[...], axis=1), axis=1, keepdims=True) * (1.0 / BW)
    coupling = jnp.concatenate([coupling, jnp.zeros((ACT - ROWS, 1), F32)], axis=0)
    high = coupling.astype(BF16).astype(F32)
    low = coupling - high
    spare = lanes((ACT, BW)) >= USED
    for k in range(GROUPS):
        tail = high if k == 0 else low if k == 1 else jnp.zeros_like(high)
        tile = jnp.where(spare, jnp.broadcast_to(tail, (ACT, BW)), fitted[:, k * BW : (k + 1) * BW])
        out_ref[:, pl.ds(k * BW, BW)] = tile.astype(BF16)


def expand_kernel(
    own_ref, one_ref, two_ref, three_ref, blocks, keep_mask, pick_mask, keep_ref, send_ref,
    coupling_ref, spread, left, coulomb, main, rest, staged,
):
    here = lax.axis_index("pair")
    core = half_here()
    along = lax.axis_index("x")
    total = (own_ref[...].astype(F32) + two_ref[...].astype(F32)) + (
        one_ref[...].astype(F32) + three_ref[...].astype(F32)
    )
    both = total[:, :BW] + total[:, BW : 2 * BW]
    coupling = jnp.sum(jnp.where(lanes((ACT, BW)) == USED, both, 0.0), axis=1, keepdims=True)
    coupling_ref[...] = jnp.broadcast_to(coupling.astype(BF16).astype(F32), (ACT, BW))
    fitted = total.astype(BF16).astype(F32)
    keep = keep_mask[...]
    for t in range(0, ACT, 2):
        pair = jnp.concatenate(
            [jnp.broadcast_to(fitted[t + d : t + d + 1, :], keep.shape) * keep for d in range(2)],
            axis=0,
        )
        spread[pl.ds(t * ACT, 2 * ACT), :] = pair.astype(BF16)
    folded = jnp.dot(
        spread[...], pick_mask[...], preferred_element_type=F32
    ).astype(BF16)
    left[...] = folded
    columns = left[pl.ds(pl.multiple_of(here * BW, BW), BW), :]
    tail = left[pl.ds(4 * BW, PAIRS - 4 * BW), :]
    main[...] = nt(folded, columns)
    rest[...] = nt(folded, jnp.concatenate([tail, tail], axis=0))
    def one(g, carry):
        total_g = jnp.zeros((BW, BW), F32)
        for p in range(ROWS):
            factor = jnp.broadcast_to(coupling_ref[pl.ds(p, 1), :], (BW, BW))
            total_g = total_g + blocks[g, p].astype(F32) * factor
        coulomb[pl.ds(pl.multiple_of(g * BW, BW), BW), :] = total_g
        return carry

    lax.fori_loop(0, SLOTS, one, 0)
    low_lane = lanes((NZ, BW)) < BW // 2
    for ref, which in ((staged, 1 - core), (keep_ref, core)):
        for step in range(NX):
            x = lax.rem(along + step, NX)
            base = step * NZ * MSG
            for z in range(NZ):
                row = pl.multiple_of(z // 2 * BW + 32 * x + 16 * which + 8 * (z % 2), 8)
                ref[pl.ds(base + z * MSG, 8), :] = coulomb[pl.ds(row, 8), :]
            first = 144 * x + 9 * which
            for s in range(9):
                ref[pl.ds(base + 8 + s, NZ, stride=MSG), :] = main[pl.ds(first + s, NZ, stride=18), :]
            for s in range(7):
                value = rest[pl.ds(first + s, NZ, stride=18), :]
                if s < 2:
                    other = rest[pl.ds(first + 7 + s, NZ, stride=18), :]
                    value = jnp.where(low_lane, value, other)
                ref[pl.ds(base + 17 + s, NZ, stride=MSG), :] = value
    send_ref[...] = staged[...].astype(BF16)


def along_x_kernel(own_ref, one_ref, two_ref, three_ref, out_ref):
    total = own_ref[...]
    for ref in (one_ref, two_ref, three_ref):
        total = total + ref[...].astype(F32)
    pieces = [total[z * MSG : (z + 1) * MSG] for z in range(NZ)]
    fock = jnp.concatenate([p[0:8] for p in pieces], axis=0).astype(BF16)
    for z in range(NZ):
        out_ref[z, 0:64, :] = fock
        out_ref[z, 64:80, :] = pieces[z][8:MSG].astype(BF16)


def route_kernel(route_ref, parts_ref, out_ref):
    total = jnp.sum(parts_ref[...].astype(F32), axis=0)
    gram = (total[64:80] * (1.0 / AUX)).astype(BF16)
    scaled = total[0:64] * (1.0 / math.sqrt(AUX))
    scaled = jnp.concatenate([scaled, jnp.zeros_like(scaled)], axis=0).astype(BF16)
    chosen = jnp.dot(route_ref[...], scaled, preferred_element_type=F32).astype(BF16)
    for o in range(OWNERS):
        for x in range(NX):
            out_ref[o * NX + x, 0:32, :] = chosen[32 * o : 32 * (o + 1)]
            out_ref[o * NX + x, 32:48, :] = gram


def place_kernel(place_ref, own_ref, other_ref, fock_out, gram_ref, fock_ref, out_sem):
    core = lax.axis_index("core")
    held = half_here()
    along = lax.axis_index("x")
    table = place_ref[...]
    for n, ref in enumerate((own_ref, other_ref)):
        which = held if n == 0 else 1 - held
        for x in range(NX):
            pieces = jnp.concatenate([ref[q * NX + x, 0:32, :] for q in range(OWNERS)], axis=0)
            placed = jnp.dot(table, pieces, preferred_element_type=F32)
            for rank in range(8):
                row = pl.multiple_of(rank * BW + 32 * x + 16 * which, 16)
                fock_ref[pl.ds(row, 16), :] = placed[16 * rank : 16 * (rank + 1)]
    copies = [
        pltpu.make_async_copy(
            fock_ref.at[pl.ds(rank * BW, BW)], fock_out.at[pl.ds(rank * BW, BW)], out_sem.at[rank]
        )
        for rank in range(8)
    ]
    for same, ref in ((True, own_ref), (False, other_ref)):

        @pl.when((held == core) == same)
        def _(ref=ref):
            for q in range(OWNERS):
                gram = ref[q * NX + along, 32:48, :].astype(F32)
                gram_ref[:, q * BW : (q + 1) * BW] = gram[0:9]
                if q == 0:
                    gram_ref[0:7, 4 * BW : PAIRS] = gram[9:16, 0 : BW // 2]
                    gram_ref[7:9, 4 * BW : PAIRS] = gram[9:11, BW // 2 : BW]
    for rank, c in enumerate(copies):
        c.start(priority=rank % 2)
    for c in copies:
        c.wait()


def from_others(x):
    return [
        lax.ppermute(x, "pair", [(i, (i + s) % OWNERS) for i in range(OWNERS)])
        for s in range(1, OWNERS)
    ]


def along(pieces):
    moved = []
    for s in range(1, NX):
        pairs = []
        for x in range(NX):
            to = (x + s) % NX
            for c in range(CORES):
                pairs.append((x * CORES + c, to * CORES + (c + flip_x(x) + flip_x(to)) % CORES))
        moved.append(lax.ppermute(pieces[s], ("x", "core"), pairs))
    return moved


def shards(three_centre, block_mask, block_owner, block_index, active_orbitals, inactive_orbitals):
    dma = pltpu.SemaphoreType.DMA
    inputs = (
        block_mask, block_owner, block_index, three_centre, active_orbitals, inactive_orbitals
    )
    pinned = [pltpu.with_memory_space_constraint(a, pltpu.HBM) for a in inputs]
    message, blocks, routes, places, keep_mask, pick_mask = pl.pallas_call(
        contract_kernel,
        out_shape=[
            pltpu.VMEM((ACT, GROUPS * BW), BF16),
            pltpu.VMEM((SLOTS, ROWS, BW, BW), BF16),
            pltpu.VMEM((BW, BW), BF16),
            pltpu.VMEM((BW, BW), BF16),
            pltpu.VMEM((ACT, GROUPS * BW), F32),
            pltpu.VMEM((GROUPS * BW, BW), BF16),
        ],
        in_specs=[HBM] * 6,
        out_specs=[VMEM] * 6,
        scratch_shapes=[
            pltpu.SMEM((16,), jnp.int32),
            pltpu.SMEM((16,), jnp.int32),
            pltpu.SMEM((2, 16), jnp.int32),
            pltpu.VMEM((ACT, NAO), BF16),
            pltpu.VMEM((NIN, NAO), BF16),
            pltpu.VMEM((BW, PER * BW), F32),
            pltpu.VMEM((SLOTS * BW, GROUPS * BW), BF16),
            pltpu.VMEM((SLOTS, BW, BW), F32),
            pltpu.VMEM((ROWS, 8, BW), F32),
            dma((3,)), dma((SLOTS,)), dma((1,)), dma((SLOTS,)),
        ],
        compiler_params=limit(8192),
        name="contract",
    )(*pinned)
    one, two, three = from_others(message)
    rows = CHIPS * MSG
    keep, send = pl.pallas_call(
        expand_kernel,
        out_shape=[pltpu.VMEM((rows, BW), F32), pltpu.VMEM((rows, BW), BF16)],
        in_specs=[VMEM] * 7,
        out_specs=[VMEM, VMEM],
        scratch_shapes=[
            pltpu.VMEM((ACT, BW), F32),
            pltpu.VMEM((PAIRS, GROUPS * BW), BF16),
            pltpu.VMEM((PAIRS, BW), BF16),
            pltpu.VMEM((SLOTS * BW, BW), F32),
            pltpu.VMEM((PAIRS, BW), F32),
            pltpu.VMEM((PAIRS, BW), F32),
            pltpu.VMEM((rows, BW), F32),
        ],
        compiler_params=limit(8192),
        name="expand",
    )(message, one, two, three, blocks, keep_mask, pick_mask)
    swap = [(0, 1), (1, 0)]
    chip_sum = (keep + lax.ppermute(send, "core", swap).astype(F32)).reshape(NX, NZ * MSG, BW)
    one, two, three = along(chip_sum.astype(BF16))
    pieces = pl.pallas_call(
        along_x_kernel,
        out_shape=pltpu.VMEM((NZ, 80, BW), BF16),
        in_specs=[VMEM] * 4,
        out_specs=VMEM,
        compiler_params=limit(4096),
        name="along_x",
    )(chip_sum[0], one, two, three)
    along_z = lax.all_to_all(pieces, "z", 0, 0, tiled=True)
    pieces = pl.pallas_call(
        route_kernel,
        out_shape=pltpu.VMEM((OWNERS * NX, 48, BW), BF16),
        in_specs=[VMEM] * 2,
        out_specs=VMEM,
        compiler_params=limit(4096),
        name="route",
    )(routes, along_z)
    received = lax.all_to_all(
        pieces, ("pair", "x", "core"), 0, 0, tiled=True, axis_index_groups=X_GROUPS
    )
    partner = lax.ppermute(received, "core", swap)
    fock, integrals = pl.pallas_call(
        place_kernel,
        out_shape=[
            jax.ShapeDtypeStruct((8 * BW, BW), F32),
            jax.ShapeDtypeStruct((9, PAIRS), F32),
        ],
        in_specs=[VMEM] * 3,
        out_specs=[HBM, VMEM],
        scratch_shapes=[pltpu.VMEM((8 * BW, BW), F32), dma((8,))],
        compiler_params=limit(4096),
        name="place",
    )(places, received, partner)
    return (fock.reshape(8, BW, BW), integrals)


def solution(mesh):
    split = Mesh(mesh.devices.reshape(NX, NZ, CORES, OWNERS), ("x", "z", "core", "pair"))
    aux = ("x", "z", "core")
    return jax.shard_map(
        shards,
        mesh=split,
        in_specs=(P("pair", aux, None, None), P(), P(), P(), P(), P()),
        out_specs=(P("pair", None, None), P(aux, None)),
        check_vma=False,
    )
```

```python
import math

import jax
import jax.numpy as jnp
from jax import lax
from jax.experimental import pallas as pl
from jax.experimental.pallas import tpu as pltpu
from jax.sharding import Mesh, PartitionSpec as P

SLOTS = 4
ROWS = 20
BW = 128
ACT = 24
PAIRS = 576
GROUPS = 4
PER = 5
USED = PER * ACT
NX = 4
NZ = 8
CHIPS = NX * NZ
CORES = 2
OWNERS = 4
AUX = 1280
NIN = 256
NAO = 3072
MSG = 24
F32 = jnp.float32
BF16 = jnp.bfloat16

HBM = pl.BlockSpec(memory_space=pltpu.HBM)
VMEM = pl.BlockSpec(memory_space=pltpu.VMEM)


def limit(kib):
    return pltpu.CompilerParams(vmem_limit_bytes=kib << 10)


def nt(a, b):
    return lax.dot_general(a, b, (((1,), (1,)), ((), ())), preferred_element_type=F32)


def lanes(shape):
    return lax.broadcasted_iota(jnp.int32, shape, len(shape) - 1)


def sublanes(shape):
    return lax.broadcasted_iota(jnp.int32, shape, len(shape) - 2)


def contract_kernel(
    mask_hbm, owner_hbm, index_hbm, blocks_hbm, active_hbm, inactive_hbm,
    out_ref, blocks, route_ref, place_ref, keep_mask, pick_mask,
    mask_ref, owner_ref, index_ref, active, inactive, wide, halves, density, sums,
    int_sem, ina_sem, act_sem, block_sem,
):
    here = lax.axis_index("pair")
    ints = [
        pltpu.make_async_copy(index_hbm, index_ref, int_sem.at[0]),
        pltpu.make_async_copy(mask_hbm, mask_ref, int_sem.at[1]),
        pltpu.make_async_copy(owner_hbm, owner_ref, int_sem.at[2]),
    ]
    part = NIN // SLOTS
    inactives = [
        pltpu.make_async_copy(
            inactive_hbm.at[pl.ds(n * part, part)], inactive.at[pl.ds(n * part, part)], ina_sem.at[n]
        )
        for n in range(SLOTS)
    ]
    actives = [pltpu.make_async_copy(active_hbm, active, act_sem.at[0])]
    whole = [
        pltpu.make_async_copy(blocks_hbm.at[g], blocks.at[g], block_sem.at[g]) for g in range(SLOTS)
    ]
    for c in ints + inactives + actives:
        c.start()
    for c in whole:
        c.start(priority=1)
    wide[...] = jnp.zeros_like(wide)
    offset = lanes((ACT, BW)) - sublanes((ACT, BW))
    keep = offset == 0
    for p in range(1, PER):
        keep = keep | (offset == ACT * p)
    keep = jnp.concatenate([keep.astype(F32)] * GROUPS, axis=1)
    keep_mask[...] = keep
    shape = (GROUPS * BW, BW)
    lane = lanes(shape)
    group = (
        (lane >= PER).astype(jnp.int32)
        + (lane >= 2 * PER).astype(jnp.int32)
        + (lane >= 3 * PER).astype(jnp.int32)
    )
    start = group * BW + (lane - group * PER) * ACT
    position = sublanes(shape) - start
    pick = (position >= 0) & (position < ACT) & (lane < ROWS)
    pick_mask[...] = pick.astype(F32).astype(BF16)
    for c in ints:
        c.wait()
    lives = [mask_ref[here * SLOTS + g] for g in range(SLOTS)]
    owners = [owner_ref[here * SLOTS + g] for g in range(SLOTS)]
    rows = [pl.multiple_of(index_ref[0, here * SLOTS + g] * BW, BW) for g in range(SLOTS)]
    cols = [pl.multiple_of(index_ref[1, here * SLOTS + g] * BW, BW) for g in range(SLOTS)]
    col = lanes((1, BW))
    at = sublanes((BW, BW))
    target = jnp.full((1, BW), -BW, jnp.int32)
    for g in range(SLOTS):
        place = jnp.int32(0)
        for h in range(g):
            place = place + jnp.where((lives[h] == 1) & (owners[h] == owners[g]), 1, 0)
        first = jnp.where(lives[g] == 1, 16 * (2 * owners[g] + place), -BW)
        inside = (col >= 16 * g) & (col < 16 * (g + 1))
        target = jnp.where(inside, first + col - 16 * g, target)
    route_ref[...] = (at == target).astype(F32).astype(BF16)
    target = jnp.full((1, BW), -BW, jnp.int32)
    rank = jnp.int32(0)
    for q in range(OWNERS):
        place = jnp.int32(0)
        firsts = [jnp.int32(-BW)] * 2
        for g in range(SLOTS):
            slot = q * SLOTS + g
            chosen = (mask_ref[slot] == 1) & (owner_ref[slot] == here)
            firsts = [jnp.where(chosen & (place == k), 16 * rank, f) for k, f in enumerate(firsts)]
            place = place + jnp.where(chosen, 1, 0)
            rank = rank + jnp.where(chosen, 1, 0)
        for k in range(2):
            begin = 16 * (2 * q + k)
            inside = (col >= begin) & (col < begin + 16)
            target = jnp.where(inside, firsts[k] + col - begin, target)
    place_ref[...] = (at == target).astype(F32).astype(BF16)
    for c in inactives:
        c.wait()
    for g in range(SLOTS):
        square = lax.dot_general(
            inactive[:, pl.ds(rows[g], BW)],
            inactive[:, pl.ds(cols[g], BW)],
            (((0,), (0,)), ((), ())),
            preferred_element_type=F32,
        )
        density[g] = square.astype(BF16).astype(F32) * lives[g].astype(F32)
    actives[0].wait()
    for g in range(SLOTS):
        column = active[:, pl.ds(cols[g], BW)].astype(F32)
        for p in range(PER):
            wide[pl.ds(ACT * p, ACT), pl.ds(BW * p, BW)] = column
        weights = wide[...].astype(BF16)
        whole[g].wait()
        for k in range(GROUPS):
            joined = jnp.concatenate([blocks[g, k * PER + p] for p in range(PER)], axis=1)
            half = nt(joined, weights)
            halves[pl.ds(g * BW, BW), pl.ds(k * BW, BW)] = half.astype(BF16)
        square = density[g]
        for p in range(ROWS):
            product = blocks[g, p].astype(F32) * square
            part_sum = jnp.sum(product.reshape(BW // 8, 8, BW), axis=0)
            if g == 0:
                sums[p] = part_sum
            else:
                sums[p] = sums[p] + part_sum
    left_side = jnp.concatenate(
        [active[:, pl.ds(rows[g], BW)].astype(F32) * lives[g].astype(F32) for g in range(SLOTS)],
        axis=1,
    ).astype(BF16)
    fitted = jnp.dot(left_side, halves[...], preferred_element_type=F32)
    coupling = jnp.sum(jnp.sum(sums[...], axis=1), axis=1, keepdims=True) * (1.0 / BW)
    coupling = jnp.concatenate([coupling, jnp.zeros((ACT - ROWS, 1), F32)], axis=0)
    high = coupling.astype(BF16).astype(F32)
    low = coupling - high
    spare = lanes((ACT, BW)) >= USED
    for k in range(GROUPS):
        tail = high if k == 0 else low if k == 1 else jnp.zeros_like(high)
        tile = jnp.where(spare, jnp.broadcast_to(tail, (ACT, BW)), fitted[:, k * BW : (k + 1) * BW])
        out_ref[:, pl.ds(k * BW, BW)] = tile.astype(BF16)


def expand_kernel(
    own_ref, one_ref, three_ref, two_ref, blocks, keep_mask, pick_mask, keep_ref, send_ref,
    coupling_ref, spread, left, coulomb, main, rest, staged,
):
    here = lax.axis_index("pair")
    core = lax.axis_index("core")
    along = lax.axis_index("x")
    total = (own_ref[...].astype(F32) + two_ref[...].astype(F32)) + (
        one_ref[...].astype(F32) + three_ref[...].astype(F32)
    )
    both = total[:, :BW] + total[:, BW : 2 * BW]
    coupling = jnp.sum(jnp.where(lanes((ACT, BW)) == USED, both, 0.0), axis=1, keepdims=True)
    coupling_ref[...] = jnp.broadcast_to(coupling.astype(BF16).astype(F32), (ACT, BW))
    fitted = total.astype(BF16).astype(F32)
    keep = keep_mask[...]
    for t in range(0, ACT, 2):
        pair = jnp.concatenate(
            [jnp.broadcast_to(fitted[t + d : t + d + 1, :], keep.shape) * keep for d in range(2)],
            axis=0,
        )
        spread[pl.ds(t * ACT, 2 * ACT), :] = pair.astype(BF16)
    folded = jnp.dot(
        spread[...], pick_mask[...], preferred_element_type=F32
    ).astype(BF16)
    left[...] = folded
    columns = left[pl.ds(pl.multiple_of(here * BW, BW), BW), :]
    tail = left[pl.ds(4 * BW, PAIRS - 4 * BW), :]
    main[...] = nt(folded, columns)
    rest[...] = nt(folded, jnp.concatenate([tail, tail], axis=0))
    def one(g, carry):
        total_g = jnp.zeros((BW, BW), F32)
        for p in range(ROWS):
            factor = jnp.broadcast_to(coupling_ref[pl.ds(p, 1), :], (BW, BW))
            total_g = total_g + blocks[g, p].astype(F32) * factor
        coulomb[pl.ds(pl.multiple_of(g * BW, BW), BW), :] = total_g
        return carry

    lax.fori_loop(0, SLOTS, one, 0)
    low_lane = lanes((NZ, BW)) < BW // 2
    for ref, which in ((staged, 1 - core), (keep_ref, core)):
        for step in range(NX):
            x = lax.rem(along + step, NX)
            base = step * NZ * MSG
            for z in range(NZ):
                row = pl.multiple_of(z // 2 * BW + 32 * x + 16 * which + 8 * (z % 2), 8)
                ref[pl.ds(base + z * MSG, 8), :] = coulomb[pl.ds(row, 8), :]
            first = 144 * x + 9 * which
            for s in range(9):
                ref[pl.ds(base + 8 + s, NZ, stride=MSG), :] = main[pl.ds(first + s, NZ, stride=18), :]
            for s in range(7):
                value = rest[pl.ds(first + s, NZ, stride=18), :]
                if s < 2:
                    other = rest[pl.ds(first + 7 + s, NZ, stride=18), :]
                    value = jnp.where(low_lane, value, other)
                ref[pl.ds(base + 17 + s, NZ, stride=MSG), :] = value
    send_ref[...] = staged[...].astype(BF16)


def along_x_kernel(own_ref, one_ref, three_ref, two_ref, out_ref):
    total = own_ref[...]
    for ref in (one_ref, two_ref, three_ref):
        total = total + ref[...].astype(F32)
    pieces = [total[z * MSG : (z + 1) * MSG] for z in range(NZ)]
    fock = jnp.concatenate([p[0:8] for p in pieces], axis=0).astype(BF16)
    for z in range(NZ):
        out_ref[z, 0:64, :] = fock
        out_ref[z, 64:80, :] = pieces[z][8:MSG].astype(BF16)


def route_kernel(route_ref, parts_ref, out_ref):
    total = jnp.sum(parts_ref[...].astype(F32), axis=0)
    gram = (total[64:80] * (1.0 / AUX)).astype(BF16)
    scaled = total[0:64] * (1.0 / math.sqrt(AUX))
    scaled = jnp.concatenate([scaled, jnp.zeros_like(scaled)], axis=0).astype(BF16)
    chosen = jnp.dot(route_ref[...], scaled, preferred_element_type=F32).astype(BF16)
    for o in range(OWNERS):
        for x in range(NX):
            out_ref[o * NX + x, 0:32, :] = chosen[32 * o : 32 * (o + 1)]
            out_ref[o * NX + x, 32:48, :] = gram


def place_kernel(place_ref, own_ref, other_ref, fock_ref, gram_ref):
    core = lax.axis_index("core")
    along = lax.axis_index("x")
    table = place_ref[...]
    for n, ref in enumerate((own_ref, other_ref)):
        which = core if n == 0 else 1 - core
        for x in range(NX):
            pieces = jnp.concatenate([ref[q * NX + x, 0:32, :] for q in range(OWNERS)], axis=0)
            placed = jnp.dot(table, pieces, preferred_element_type=F32)
            for rank in range(8):
                row = pl.multiple_of(rank * BW + 32 * x + 16 * which, 16)
                fock_ref[pl.ds(row, 16), :] = placed[16 * rank : 16 * (rank + 1)]
    for q in range(OWNERS):
        gram = own_ref[q * NX + along, 32:48, :].astype(F32)
        gram_ref[:, q * BW : (q + 1) * BW] = gram[0:9]
        if q == 0:
            gram_ref[0:7, 4 * BW : PAIRS] = gram[9:16, 0 : BW // 2]
            gram_ref[7:9, 4 * BW : PAIRS] = gram[9:11, BW // 2 : BW]


def from_others(x, axis="pair"):
    moved = {
        s: lax.ppermute(x if axis == "pair" else x[s], axis, [(i, (i + s) % 4) for i in range(4)])
        for s in (1, 3, 2)
    }
    return [moved[s] for s in range(1, 4)]


def shards(three_centre, block_mask, block_owner, block_index, active_orbitals, inactive_orbitals):
    dma = pltpu.SemaphoreType.DMA
    inputs = (
        block_mask, block_owner, block_index, three_centre, active_orbitals, inactive_orbitals
    )
    pinned = [pltpu.with_memory_space_constraint(a, pltpu.HBM) for a in inputs]
    message, blocks, routes, places, keep_mask, pick_mask = pl.pallas_call(
        contract_kernel,
        out_shape=[
            pltpu.VMEM((ACT, GROUPS * BW), BF16),
            pltpu.VMEM((SLOTS, ROWS, BW, BW), BF16),
            pltpu.VMEM((BW, BW), BF16),
            pltpu.VMEM((BW, BW), BF16),
            pltpu.VMEM((ACT, GROUPS * BW), F32),
            pltpu.VMEM((GROUPS * BW, BW), BF16),
        ],
        in_specs=[HBM] * 6,
        out_specs=[VMEM] * 6,
        scratch_shapes=[
            pltpu.SMEM((16,), jnp.int32),
            pltpu.SMEM((16,), jnp.int32),
            pltpu.SMEM((2, 16), jnp.int32),
            pltpu.VMEM((ACT, NAO), BF16),
            pltpu.VMEM((NIN, NAO), BF16),
            pltpu.VMEM((BW, PER * BW), F32),
            pltpu.VMEM((SLOTS * BW, GROUPS * BW), BF16),
            pltpu.VMEM((SLOTS, BW, BW), F32),
            pltpu.VMEM((ROWS, 8, BW), F32),
            dma((3,)), dma((SLOTS,)), dma((1,)), dma((SLOTS,)),
        ],
        compiler_params=limit(8192),
        name="contract",
    )(*pinned)
    one, two, three = from_others(message)
    rows = CHIPS * MSG
    keep, send = pl.pallas_call(
        expand_kernel,
        out_shape=[pltpu.VMEM((rows, BW), F32), pltpu.VMEM((rows, BW), BF16)],
        in_specs=[VMEM] * 7,
        out_specs=[VMEM, VMEM],
        scratch_shapes=[
            pltpu.VMEM((ACT, BW), F32),
            pltpu.VMEM((PAIRS, GROUPS * BW), BF16),
            pltpu.VMEM((PAIRS, BW), BF16),
            pltpu.VMEM((SLOTS * BW, BW), F32),
            pltpu.VMEM((PAIRS, BW), F32),
            pltpu.VMEM((PAIRS, BW), F32),
            pltpu.VMEM((rows, BW), F32),
        ],
        compiler_params=limit(8192),
        name="expand",
    )(message, one, three, two, blocks, keep_mask, pick_mask)
    swap = [(0, 1), (1, 0)]
    chip_sum = (keep + lax.ppermute(send, "core", swap).astype(F32)).reshape(NX, NZ * MSG, BW)
    one, two, three = from_others(chip_sum.astype(BF16), "x")
    pieces = pl.pallas_call(
        along_x_kernel,
        out_shape=pltpu.VMEM((NZ, 80, BW), BF16),
        in_specs=[VMEM] * 4,
        out_specs=VMEM,
        compiler_params=limit(4096),
        name="along_x",
    )(chip_sum[0], one, three, two)
    along_z = lax.all_to_all(pieces, "z", 0, 0, tiled=True)
    pieces = pl.pallas_call(
        route_kernel,
        out_shape=pltpu.VMEM((OWNERS * NX, 48, BW), BF16),
        in_specs=[VMEM] * 2,
        out_specs=VMEM,
        compiler_params=limit(4096),
        name="route",
    )(routes, along_z)
    received = lax.all_to_all(pieces, ("pair", "x"), 0, 0, tiled=True)
    partner = lax.ppermute(received, "core", swap)
    fock, integrals = pl.pallas_call(
        place_kernel,
        out_shape=[
            jax.ShapeDtypeStruct((8 * BW, BW), F32),
            jax.ShapeDtypeStruct((9, PAIRS), F32),
        ],
        in_specs=[VMEM] * 3,
        out_specs=[VMEM, VMEM],
        compiler_params=limit(4096),
        name="place",
    )(places, received, partner)
    return (fock.reshape(8, BW, BW), integrals)


def solution(mesh):
    split = Mesh(mesh.devices.reshape(NX, NZ, CORES, OWNERS), ("x", "z", "core", "pair"))
    aux = ("x", "z", "core")
    return jax.shard_map(
        shards,
        mesh=split,
        in_specs=(P("pair", aux, None, None), P(), P(), P(), P(), P()),
        out_specs=(P("pair", None, None), P(aux, None)),
        check_vma=False,
    )
```

```python
import math

import jax
import jax.numpy as jnp
from jax import lax
from jax.experimental import pallas as pl
from jax.experimental.pallas import tpu as pltpu
from jax.sharding import Mesh, PartitionSpec as P

SLOTS = 4
ROWS = 20
BW = 128
ACT = 24
PAIRS = 576
GROUPS = 4
PER = 5
USED = PER * ACT
NX = 4
NZ = 8
CHIPS = NX * NZ
CORES = 2
OWNERS = 4
AUX = 1280
NIN = 256
NAO = 3072
MSG = 24
F32 = jnp.float32
BF16 = jnp.bfloat16

HBM = pl.BlockSpec(memory_space=pltpu.HBM)
VMEM = pl.BlockSpec(memory_space=pltpu.VMEM)


def limit(kib):
    return pltpu.CompilerParams(vmem_limit_bytes=kib << 10)


def nt(a, b):
    return lax.dot_general(a, b, (((1,), (1,)), ((), ())), preferred_element_type=F32)


def lanes(shape):
    return lax.broadcasted_iota(jnp.int32, shape, len(shape) - 1)


def sublanes(shape):
    return lax.broadcasted_iota(jnp.int32, shape, len(shape) - 2)


def contract_kernel(
    mask_hbm, owner_hbm, index_hbm, blocks_hbm, active_hbm, inactive_hbm,
    out_ref, blocks, route_ref, place_ref, keep_mask, pick_mask,
    mask_ref, owner_ref, index_ref, active, inactive, wide, halves, density, sums,
    int_sem, ina_sem, act_sem, block_sem,
):
    here = lax.axis_index("pair")
    ints = [
        pltpu.make_async_copy(index_hbm, index_ref, int_sem.at[0]),
        pltpu.make_async_copy(mask_hbm, mask_ref, int_sem.at[1]),
        pltpu.make_async_copy(owner_hbm, owner_ref, int_sem.at[2]),
    ]
    part = NIN // SLOTS
    inactives = [
        pltpu.make_async_copy(
            inactive_hbm.at[pl.ds(n * part, part)], inactive.at[pl.ds(n * part, part)], ina_sem.at[n]
        )
        for n in range(SLOTS)
    ]
    actives = [pltpu.make_async_copy(active_hbm, active, act_sem.at[0])]
    whole = [
        pltpu.make_async_copy(blocks_hbm.at[g], blocks.at[g], block_sem.at[g]) for g in range(SLOTS)
    ]
    for c in ints + inactives + actives:
        c.start()
    for c in whole:
        c.start(priority=1)
    wide[...] = jnp.zeros_like(wide)
    offset = lanes((ACT, BW)) - sublanes((ACT, BW))
    keep = offset == 0
    for p in range(1, PER):
        keep = keep | (offset == ACT * p)
    keep = jnp.concatenate([keep.astype(F32)] * GROUPS, axis=1)
    keep_mask[...] = keep
    shape = (GROUPS * BW, BW)
    lane = lanes(shape)
    group = (
        (lane >= PER).astype(jnp.int32)
        + (lane >= 2 * PER).astype(jnp.int32)
        + (lane >= 3 * PER).astype(jnp.int32)
    )
    start = group * BW + (lane - group * PER) * ACT
    position = sublanes(shape) - start
    pick = (position >= 0) & (position < ACT) & (lane < ROWS)
    pick_mask[...] = pick.astype(F32).astype(BF16)
    for c in ints:
        c.wait()
    lives = [mask_ref[here * SLOTS + g] for g in range(SLOTS)]
    owners = [owner_ref[here * SLOTS + g] for g in range(SLOTS)]
    rows = [pl.multiple_of(index_ref[0, here * SLOTS + g] * BW, BW) for g in range(SLOTS)]
    cols = [pl.multiple_of(index_ref[1, here * SLOTS + g] * BW, BW) for g in range(SLOTS)]
    col = lanes((1, BW))
    at = sublanes((BW, BW))
    target = jnp.full((1, BW), -BW, jnp.int32)
    for g in range(SLOTS):
        place = jnp.int32(0)
        for h in range(g):
            place = place + jnp.where((lives[h] == 1) & (owners[h] == owners[g]), 1, 0)
        first = jnp.where(lives[g] == 1, 16 * (2 * owners[g] + place), -BW)
        inside = (col >= 16 * g) & (col < 16 * (g + 1))
        target = jnp.where(inside, first + col - 16 * g, target)
    route_ref[...] = (at == target).astype(F32).astype(BF16)
    target = jnp.full((1, BW), -BW, jnp.int32)
    rank = jnp.int32(0)
    for q in range(OWNERS):
        place = jnp.int32(0)
        firsts = [jnp.int32(-BW)] * 2
        for g in range(SLOTS):
            slot = q * SLOTS + g
            chosen = (mask_ref[slot] == 1) & (owner_ref[slot] == here)
            firsts = [jnp.where(chosen & (place == k), 16 * rank, f) for k, f in enumerate(firsts)]
            place = place + jnp.where(chosen, 1, 0)
            rank = rank + jnp.where(chosen, 1, 0)
        for k in range(2):
            begin = 16 * (2 * q + k)
            inside = (col >= begin) & (col < begin + 16)
            target = jnp.where(inside, firsts[k] + col - begin, target)
    place_ref[...] = (at == target).astype(F32).astype(BF16)
    for c in inactives:
        c.wait()
    for g in range(SLOTS):
        square = lax.dot_general(
            inactive[:, pl.ds(rows[g], BW)],
            inactive[:, pl.ds(cols[g], BW)],
            (((0,), (0,)), ((), ())),
            preferred_element_type=F32,
        )
        density[g] = square.astype(BF16).astype(F32) * lives[g].astype(F32)
    actives[0].wait()
    for g in range(SLOTS):
        column = active[:, pl.ds(cols[g], BW)].astype(F32)
        for p in range(PER):
            wide[pl.ds(ACT * p, ACT), pl.ds(BW * p, BW)] = column
        weights = wide[...].astype(BF16)
        whole[g].wait()
        for k in range(GROUPS):
            joined = jnp.concatenate([blocks[g, k * PER + p] for p in range(PER)], axis=1)
            half = nt(joined, weights)
            halves[pl.ds(g * BW, BW), pl.ds(k * BW, BW)] = half.astype(BF16)
        square = density[g]
        for p in range(ROWS):
            product = blocks[g, p].astype(F32) * square
            part_sum = jnp.sum(product.reshape(BW // 8, 8, BW), axis=0)
            if g == 0:
                sums[p] = part_sum
            else:
                sums[p] = sums[p] + part_sum
    left_side = jnp.concatenate(
        [active[:, pl.ds(rows[g], BW)].astype(F32) * lives[g].astype(F32) for g in range(SLOTS)],
        axis=1,
    ).astype(BF16)
    fitted = jnp.dot(left_side, halves[...], preferred_element_type=F32)
    coupling = jnp.sum(jnp.sum(sums[...], axis=1), axis=1, keepdims=True) * (1.0 / BW)
    coupling = jnp.concatenate([coupling, jnp.zeros((ACT - ROWS, 1), F32)], axis=0)
    high = coupling.astype(BF16).astype(F32)
    low = coupling - high
    spare = lanes((ACT, BW)) >= USED
    for k in range(GROUPS):
        tail = high if k == 0 else low if k == 1 else jnp.zeros_like(high)
        tile = jnp.where(spare, jnp.broadcast_to(tail, (ACT, BW)), fitted[:, k * BW : (k + 1) * BW])
        out_ref[:, pl.ds(k * BW, BW)] = tile.astype(BF16)


def expand_kernel(
    own_ref, one_ref, two_ref, three_ref, blocks, keep_mask, pick_mask, keep_ref, send_ref,
    coupling_ref, spread, left, coulomb, main, rest, staged,
):
    here = lax.axis_index("pair")
    core = lax.axis_index("core")
    along = lax.axis_index("x")
    total = (own_ref[...].astype(F32) + two_ref[...].astype(F32)) + (
        one_ref[...].astype(F32) + three_ref[...].astype(F32)
    )
    both = total[:, :BW] + total[:, BW : 2 * BW]
    coupling = jnp.sum(jnp.where(lanes((ACT, BW)) == USED, both, 0.0), axis=1, keepdims=True)
    coupling_ref[...] = jnp.broadcast_to(coupling.astype(BF16).astype(F32), (ACT, BW))
    fitted = total.astype(BF16).astype(F32)
    keep = keep_mask[...]
    for t in range(0, ACT, 2):
        pair = jnp.concatenate(
            [jnp.broadcast_to(fitted[t + d : t + d + 1, :], keep.shape) * keep for d in range(2)],
            axis=0,
        )
        spread[pl.ds(t * ACT, 2 * ACT), :] = pair.astype(BF16)
    folded = jnp.dot(
        spread[...], pick_mask[...], preferred_element_type=F32
    ).astype(BF16)
    left[...] = folded
    columns = left[pl.ds(pl.multiple_of(here * BW, BW), BW), :]
    tail = left[pl.ds(4 * BW, PAIRS - 4 * BW), :]
    main[...] = nt(folded, columns)
    rest[...] = nt(folded, jnp.concatenate([tail, tail], axis=0))
    def one(g, carry):
        total_g = jnp.zeros((BW, BW), F32)
        for p in range(ROWS):
            factor = jnp.broadcast_to(coupling_ref[pl.ds(p, 1), :], (BW, BW))
            total_g = total_g + blocks[g, p].astype(F32) * factor
        coulomb[pl.ds(pl.multiple_of(g * BW, BW), BW), :] = total_g
        return carry

    lax.fori_loop(0, SLOTS, one, 0)
    low_lane = lanes((NZ, BW)) < BW // 2
    for ref, which in ((staged, 1 - core), (keep_ref, core)):
        for step in range(NX):
            x = lax.rem(along + step, NX)
            base = step * NZ * MSG
            for z in range(NZ):
                row = pl.multiple_of(z // 2 * BW + 32 * x + 16 * which + 8 * (z % 2), 8)
                ref[pl.ds(base + z * MSG, 8), :] = coulomb[pl.ds(row, 8), :]
            first = 144 * x + 9 * which
            for s in range(9):
                ref[pl.ds(base + 8 + s, NZ, stride=MSG), :] = main[pl.ds(first + s, NZ, stride=18), :]
            for s in range(7):
                value = rest[pl.ds(first + s, NZ, stride=18), :]
                if s < 2:
                    other = rest[pl.ds(first + 7 + s, NZ, stride=18), :]
                    value = jnp.where(low_lane, value, other)
                ref[pl.ds(base + 17 + s, NZ, stride=MSG), :] = value
    send_ref[...] = staged[...].astype(BF16)


def along_x_kernel(own_ref, one_ref, two_ref, three_ref, out_ref):
    total = own_ref[...]
    for ref in (one_ref, two_ref, three_ref):
        total = total + ref[...].astype(F32)
    pieces = [total[z * MSG : (z + 1) * MSG] for z in range(NZ)]
    fock = jnp.concatenate([p[0:8] for p in pieces], axis=0).astype(BF16)
    for z in range(NZ):
        out_ref[z, 0:64, :] = fock
        out_ref[z, 64:80, :] = pieces[z][8:MSG].astype(BF16)


def route_kernel(route_ref, parts_ref, out_ref):
    total = jnp.sum(parts_ref[...].astype(F32), axis=0)
    gram = (total[64:80] * (1.0 / AUX)).astype(BF16)
    scaled = total[0:64] * (1.0 / math.sqrt(AUX))
    scaled = jnp.concatenate([scaled, jnp.zeros_like(scaled)], axis=0).astype(BF16)
    chosen = jnp.dot(route_ref[...], scaled, preferred_element_type=F32).astype(BF16)
    for o in range(OWNERS):
        for x in range(NX):
            for c in range(CORES):
                to = (o * NX + x) * CORES + c
                out_ref[to, 0:32, :] = chosen[32 * o : 32 * (o + 1)]
                out_ref[to, 32:48, :] = gram


def place_kernel(place_ref, ref, fock_ref, gram_ref):
    core = lax.axis_index("core")
    along = lax.axis_index("x")
    table = place_ref[...]
    for c in range(CORES):
        for x in range(NX):
            pieces = jnp.concatenate(
                [ref[(q * NX + x) * CORES + c, 0:32, :] for q in range(OWNERS)], axis=0
            )
            placed = jnp.dot(table, pieces, preferred_element_type=F32)
            for rank in range(8):
                row = rank * BW + 32 * x + 16 * c
                fock_ref[row : row + 16, :] = placed[16 * rank : 16 * (rank + 1)]
    for q in range(OWNERS):
        gram = ref[(q * NX + along) * CORES + core, 32:48, :].astype(F32)
        gram_ref[:, q * BW : (q + 1) * BW] = gram[0:9]
        if q == 0:
            gram_ref[0:7, 4 * BW : PAIRS] = gram[9:16, 0 : BW // 2]
            gram_ref[7:9, 4 * BW : PAIRS] = gram[9:11, BW // 2 : BW]


def from_others(x, axis="pair"):
    return [
        lax.ppermute(x if axis == "pair" else x[s], axis, [(i, (i + s) % 4) for i in range(4)])
        for s in range(1, 4)
    ]


def shards(three_centre, block_mask, block_owner, block_index, active_orbitals, inactive_orbitals):
    dma = pltpu.SemaphoreType.DMA
    inputs = (
        block_mask, block_owner, block_index, three_centre, active_orbitals, inactive_orbitals
    )
    pinned = [pltpu.with_memory_space_constraint(a, pltpu.HBM) for a in inputs]
    message, blocks, routes, places, keep_mask, pick_mask = pl.pallas_call(
        contract_kernel,
        out_shape=[
            pltpu.VMEM((ACT, GROUPS * BW), BF16),
            pltpu.VMEM((SLOTS, ROWS, BW, BW), BF16),
            pltpu.VMEM((BW, BW), BF16),
            pltpu.VMEM((BW, BW), BF16),
            pltpu.VMEM((ACT, GROUPS * BW), F32),
            pltpu.VMEM((GROUPS * BW, BW), BF16),
        ],
        in_specs=[HBM] * 6,
        out_specs=[VMEM] * 6,
        scratch_shapes=[
            pltpu.SMEM((16,), jnp.int32),
            pltpu.SMEM((16,), jnp.int32),
            pltpu.SMEM((2, 16), jnp.int32),
            pltpu.VMEM((ACT, NAO), BF16),
            pltpu.VMEM((NIN, NAO), BF16),
            pltpu.VMEM((BW, PER * BW), F32),
            pltpu.VMEM((SLOTS * BW, GROUPS * BW), BF16),
            pltpu.VMEM((SLOTS, BW, BW), F32),
            pltpu.VMEM((ROWS, 8, BW), F32),
            dma((3,)), dma((SLOTS,)), dma((1,)), dma((SLOTS,)),
        ],
        compiler_params=limit(8192),
        name="contract",
    )(*pinned)
    one, two, three = from_others(message)
    rows = CHIPS * MSG
    keep, send = pl.pallas_call(
        expand_kernel,
        out_shape=[pltpu.VMEM((rows, BW), F32), pltpu.VMEM((rows, BW), BF16)],
        in_specs=[VMEM] * 7,
        out_specs=[VMEM, VMEM],
        scratch_shapes=[
            pltpu.VMEM((ACT, BW), F32),
            pltpu.VMEM((PAIRS, GROUPS * BW), BF16),
            pltpu.VMEM((PAIRS, BW), BF16),
            pltpu.VMEM((SLOTS * BW, BW), F32),
            pltpu.VMEM((PAIRS, BW), F32),
            pltpu.VMEM((PAIRS, BW), F32),
            pltpu.VMEM((rows, BW), F32),
        ],
        compiler_params=limit(8192),
        name="expand",
    )(message, one, two, three, blocks, keep_mask, pick_mask)
    swap = [(0, 1), (1, 0)]
    chip_sum = (keep + lax.ppermute(send, "core", swap).astype(F32)).reshape(NX, NZ * MSG, BW)
    one, two, three = from_others(chip_sum.astype(BF16), "x")
    pieces = pl.pallas_call(
        along_x_kernel,
        out_shape=pltpu.VMEM((NZ, 80, BW), BF16),
        in_specs=[VMEM] * 4,
        out_specs=VMEM,
        compiler_params=limit(4096),
        name="along_x",
    )(chip_sum[0], one, two, three)
    along_z = lax.all_to_all(pieces, "z", 0, 0, tiled=True)
    pieces = pl.pallas_call(
        route_kernel,
        out_shape=pltpu.VMEM((OWNERS * NX * CORES, 48, BW), BF16),
        in_specs=[VMEM] * 2,
        out_specs=VMEM,
        compiler_params=limit(4096),
        name="route",
    )(routes, along_z)
    received = lax.all_to_all(pieces, ("pair", "x", "core"), 0, 0, tiled=True)
    fock, integrals = pl.pallas_call(
        place_kernel,
        out_shape=[
            jax.ShapeDtypeStruct((8 * BW, BW), F32),
            jax.ShapeDtypeStruct((9, PAIRS), F32),
        ],
        in_specs=[VMEM] * 2,
        out_specs=[VMEM, VMEM],
        compiler_params=limit(4096),
        name="place",
    )(places, received)
    return (fock.reshape(8, BW, BW), integrals)


def solution(mesh):
    split = Mesh(mesh.devices.reshape(NX, NZ, CORES, OWNERS), ("x", "z", "core", "pair"))
    aux = ("x", "z", "core")
    return jax.shard_map(
        shards,
        mesh=split,
        in_specs=(P("pair", aux, None, None), P(), P(), P(), P(), P()),
        out_specs=(P("pair", None, None), P(aux, None)),
        check_vma=False,
    )
```

```python
import math

import jax
import jax.numpy as jnp
from jax import lax
from jax.experimental import pallas as pl
from jax.experimental.pallas import tpu as pltpu
from jax.sharding import Mesh, PartitionSpec as P

SLOTS = 4
ROWS = 20
BW = 128
ACT = 24
PAIRS = 576
GROUPS = 4
PER = 5
USED = PER * ACT
NX = 4
NZ = 8
CHIPS = NX * NZ
CORES = 2
OWNERS = 4
AUX = 1280
NIN = 256
NAO = 3072
MSG = 24
F32 = jnp.float32
BF16 = jnp.bfloat16

HBM = pl.BlockSpec(memory_space=pltpu.HBM)
VMEM = pl.BlockSpec(memory_space=pltpu.VMEM)


def limit(kib):
    return pltpu.CompilerParams(vmem_limit_bytes=kib << 10)


def nt(a, b):
    return lax.dot_general(a, b, (((1,), (1,)), ((), ())), preferred_element_type=F32)


def lanes(shape):
    return lax.broadcasted_iota(jnp.int32, shape, len(shape) - 1)


def sublanes(shape):
    return lax.broadcasted_iota(jnp.int32, shape, len(shape) - 2)


def contract_kernel(
    mask_hbm, owner_hbm, index_hbm, blocks_hbm, active_hbm, inactive_hbm,
    out_ref, blocks, route_ref, place_ref, keep_mask, pick_mask,
    mask_ref, owner_ref, index_ref, active, inactive, wide, halves, density, sums,
    int_sem, ina_sem, act_sem, block_sem,
):
    here = lax.axis_index("pair")
    ints = [
        pltpu.make_async_copy(index_hbm, index_ref, int_sem.at[0]),
        pltpu.make_async_copy(mask_hbm, mask_ref, int_sem.at[1]),
        pltpu.make_async_copy(owner_hbm, owner_ref, int_sem.at[2]),
    ]
    part = NIN // SLOTS
    inactives = [
        pltpu.make_async_copy(
            inactive_hbm.at[pl.ds(n * part, part)], inactive.at[pl.ds(n * part, part)], ina_sem.at[n]
        )
        for n in range(SLOTS)
    ]
    actives = [pltpu.make_async_copy(active_hbm, active, act_sem.at[0])]
    whole = [
        pltpu.make_async_copy(blocks_hbm.at[g], blocks.at[g], block_sem.at[g]) for g in range(SLOTS)
    ]
    for c in ints + inactives + actives:
        c.start()
    for c in whole:
        c.start(priority=1)
    wide[...] = jnp.zeros_like(wide)
    offset = lanes((ACT, BW)) - sublanes((ACT, BW))
    keep = offset == 0
    for p in range(1, PER):
        keep = keep | (offset == ACT * p)
    keep = jnp.concatenate([keep.astype(F32)] * GROUPS, axis=1)
    keep_mask[...] = keep
    shape = (GROUPS * BW, BW)
    lane = lanes(shape)
    group = (
        (lane >= PER).astype(jnp.int32)
        + (lane >= 2 * PER).astype(jnp.int32)
        + (lane >= 3 * PER).astype(jnp.int32)
    )
    start = group * BW + (lane - group * PER) * ACT
    position = sublanes(shape) - start
    pick = (position >= 0) & (position < ACT) & (lane < ROWS)
    pick_mask[...] = pick.astype(F32).astype(BF16)
    for c in ints:
        c.wait()
    lives = [mask_ref[here * SLOTS + g] for g in range(SLOTS)]
    owners = [owner_ref[here * SLOTS + g] for g in range(SLOTS)]
    rows = [pl.multiple_of(index_ref[0, here * SLOTS + g] * BW, BW) for g in range(SLOTS)]
    cols = [pl.multiple_of(index_ref[1, here * SLOTS + g] * BW, BW) for g in range(SLOTS)]
    col = lanes((1, BW))
    at = sublanes((BW, BW))
    target = jnp.full((1, BW), -BW, jnp.int32)
    for g in range(SLOTS):
        place = jnp.int32(0)
        for h in range(g):
            place = place + jnp.where((lives[h] == 1) & (owners[h] == owners[g]), 1, 0)
        first = jnp.where(lives[g] == 1, 16 * (2 * owners[g] + place), -BW)
        inside = (col >= 16 * g) & (col < 16 * (g + 1))
        target = jnp.where(inside, first + col - 16 * g, target)
    route_ref[...] = (at == target).astype(F32).astype(BF16)
    target = jnp.full((1, BW), -BW, jnp.int32)
    rank = jnp.int32(0)
    for q in range(OWNERS):
        place = jnp.int32(0)
        firsts = [jnp.int32(-BW)] * 2
        for g in range(SLOTS):
            slot = q * SLOTS + g
            chosen = (mask_ref[slot] == 1) & (owner_ref[slot] == here)
            firsts = [jnp.where(chosen & (place == k), 16 * rank, f) for k, f in enumerate(firsts)]
            place = place + jnp.where(chosen, 1, 0)
            rank = rank + jnp.where(chosen, 1, 0)
        for k in range(2):
            begin = 16 * (2 * q + k)
            inside = (col >= begin) & (col < begin + 16)
            target = jnp.where(inside, firsts[k] + col - begin, target)
    place_ref[...] = (at == target).astype(F32).astype(BF16)
    for c in inactives:
        c.wait()
    for g in range(SLOTS):
        square = lax.dot_general(
            inactive[:, pl.ds(rows[g], BW)],
            inactive[:, pl.ds(cols[g], BW)],
            (((0,), (0,)), ((), ())),
            preferred_element_type=F32,
        )
        density[g] = square.astype(BF16).astype(F32) * lives[g].astype(F32)
    actives[0].wait()
    for g in range(SLOTS):
        column = active[:, pl.ds(cols[g], BW)].astype(F32)
        for p in range(PER):
            wide[pl.ds(ACT * p, ACT), pl.ds(BW * p, BW)] = column
        weights = wide[...].astype(BF16)
        whole[g].wait()
        for k in range(GROUPS):
            joined = jnp.concatenate([blocks[g, k * PER + p] for p in range(PER)], axis=1)
            half = nt(joined, weights)
            halves[pl.ds(g * BW, BW), pl.ds(k * BW, BW)] = half.astype(BF16)
        square = density[g]
        for p in range(ROWS):
            product = blocks[g, p].astype(F32) * square
            part_sum = jnp.sum(product.reshape(BW // 8, 8, BW), axis=0)
            if g == 0:
                sums[p] = part_sum
            else:
                sums[p] = sums[p] + part_sum
    left_side = jnp.concatenate(
        [active[:, pl.ds(rows[g], BW)].astype(F32) * lives[g].astype(F32) for g in range(SLOTS)],
        axis=1,
    ).astype(BF16)
    fitted = jnp.dot(left_side, halves[...], preferred_element_type=F32)
    coupling = jnp.sum(jnp.sum(sums[...], axis=1), axis=1, keepdims=True) * (1.0 / BW)
    coupling = jnp.concatenate([coupling, jnp.zeros((ACT - ROWS, 1), F32)], axis=0)
    high = coupling.astype(BF16).astype(F32)
    low = coupling - high
    spare = lanes((ACT, BW)) >= USED
    for k in range(GROUPS):
        tail = high if k == 0 else low if k == 1 else jnp.zeros_like(high)
        tile = jnp.where(spare, jnp.broadcast_to(tail, (ACT, BW)), fitted[:, k * BW : (k + 1) * BW])
        out_ref[:, pl.ds(k * BW, BW)] = tile.astype(BF16)


def expand_kernel(
    own_ref, one_ref, two_ref, three_ref, blocks, keep_mask, pick_mask, keep_ref, send_ref,
    coupling_ref, spread, left, coulomb, main, rest, staged,
):
    here = lax.axis_index("pair")
    core = lax.axis_index("core")
    along = lax.axis_index("x")
    total = (own_ref[...].astype(F32) + two_ref[...].astype(F32)) + (
        one_ref[...].astype(F32) + three_ref[...].astype(F32)
    )
    both = total[:, :BW] + total[:, BW : 2 * BW]
    coupling = jnp.sum(jnp.where(lanes((ACT, BW)) == USED, both, 0.0), axis=1, keepdims=True)
    coupling_ref[...] = jnp.broadcast_to(coupling.astype(BF16).astype(F32), (ACT, BW))
    fitted = total.astype(BF16).astype(F32)
    keep = keep_mask[...]
    for t in range(0, ACT, 2):
        pair = jnp.concatenate(
            [jnp.broadcast_to(fitted[t + d : t + d + 1, :], keep.shape) * keep for d in range(2)],
            axis=0,
        )
        spread[pl.ds(t * ACT, 2 * ACT), :] = pair.astype(BF16)
    folded = jnp.dot(
        spread[...], pick_mask[...], preferred_element_type=F32
    ).astype(BF16)
    left[...] = folded
    columns = left[pl.ds(pl.multiple_of(here * BW, BW), BW), :]
    tail = left[pl.ds(4 * BW, PAIRS - 4 * BW), :]
    main[...] = nt(folded, columns)
    rest[...] = nt(folded, jnp.concatenate([tail, tail], axis=0))
    def one(g, carry):
        total_g = jnp.zeros((BW, BW), F32)
        for p in range(ROWS):
            factor = jnp.broadcast_to(coupling_ref[pl.ds(p, 1), :], (BW, BW))
            total_g = total_g + blocks[g, p].astype(F32) * factor
        coulomb[pl.ds(pl.multiple_of(g * BW, BW), BW), :] = total_g
        return carry

    lax.fori_loop(0, SLOTS, one, 0)
    low_lane = lanes((NZ, BW)) < BW // 2
    for ref, which in ((staged, 1 - core), (keep_ref, core)):
        for step in range(NX):
            x = lax.rem(along + step, NX)
            base = step * NZ * MSG
            for z in range(NZ):
                row = pl.multiple_of(z // 2 * BW + 32 * x + 16 * which + 8 * (z % 2), 8)
                ref[pl.ds(base + z * MSG, 8), :] = coulomb[pl.ds(row, 8), :]
            first = 144 * x + 9 * which
            for s in range(9):
                ref[pl.ds(base + 8 + s, NZ, stride=MSG), :] = main[pl.ds(first + s, NZ, stride=18), :]
            for s in range(7):
                value = rest[pl.ds(first + s, NZ, stride=18), :]
                if s < 2:
                    other = rest[pl.ds(first + 7 + s, NZ, stride=18), :]
                    value = jnp.where(low_lane, value, other)
                ref[pl.ds(base + 17 + s, NZ, stride=MSG), :] = value
    send_ref[...] = staged[...].astype(BF16)


def along_x_kernel(own_ref, one_ref, two_ref, three_ref, out_ref):
    total = own_ref[...]
    for ref in (one_ref, two_ref, three_ref):
        total = total + ref[...].astype(F32)
    pieces = [total[z * MSG : (z + 1) * MSG] for z in range(NZ)]
    fock = jnp.concatenate([p[0:8] for p in pieces], axis=0).astype(BF16)
    for z in range(NZ):
        out_ref[z, 0:64, :] = fock
        out_ref[z, 64:80, :] = pieces[z][8:MSG].astype(BF16)


def route_kernel(route_ref, parts_ref, out_ref):
    total = jnp.sum(parts_ref[...].astype(F32), axis=0)
    gram = (total[64:80] * (1.0 / AUX)).astype(BF16)
    scaled = total[0:64] * (1.0 / math.sqrt(AUX))
    scaled = jnp.concatenate([scaled, jnp.zeros_like(scaled)], axis=0).astype(BF16)
    chosen = jnp.dot(route_ref[...], scaled, preferred_element_type=F32).astype(BF16)
    for o in range(OWNERS):
        for x in range(NX):
            out_ref[o * NX + x, 0:32, :] = chosen[32 * o : 32 * (o + 1)]
            out_ref[o * NX + x, 32:48, :] = gram


def place_kernel(place_ref, own_ref, other_ref, fock_ref, gram_ref):
    core = lax.axis_index("core")
    along = lax.axis_index("x")
    table = place_ref[...]
    for n, ref in enumerate((own_ref, other_ref)):
        which = core if n == 0 else 1 - core
        for x in range(NX):
            pieces = jnp.concatenate([ref[q * NX + x, 0:32, :] for q in range(OWNERS)], axis=0)
            placed = jnp.dot(table, pieces, preferred_element_type=F32)
            for rank in range(8):
                row = pl.multiple_of(rank * BW + 32 * x + 16 * which, 16)
                fock_ref[pl.ds(row, 16), :] = placed[16 * rank : 16 * (rank + 1)]
    for q in range(OWNERS):
        gram = own_ref[q * NX + along, 32:48, :].astype(F32)
        gram_ref[:, q * BW : (q + 1) * BW] = gram[0:9]
        if q == 0:
            gram_ref[0:7, 4 * BW : PAIRS] = gram[9:16, 0 : BW // 2]
            gram_ref[7:9, 4 * BW : PAIRS] = gram[9:11, BW // 2 : BW]


def from_others(x, axis="pair"):
    return [
        lax.ppermute(x if axis == "pair" else x[s], axis, [(i, (i + s) % 4) for i in range(4)])
        for s in range(1, 4)
    ]


def shards(three_centre, block_mask, block_owner, block_index, active_orbitals, inactive_orbitals):
    dma = pltpu.SemaphoreType.DMA
    inputs = (
        block_mask, block_owner, block_index, three_centre, active_orbitals, inactive_orbitals
    )
    pinned = [pltpu.with_memory_space_constraint(a, pltpu.HBM) for a in inputs]
    message, blocks, routes, places, keep_mask, pick_mask = pl.pallas_call(
        contract_kernel,
        out_shape=[
            pltpu.VMEM((ACT, GROUPS * BW), BF16),
            pltpu.VMEM((SLOTS, ROWS, BW, BW), BF16),
            pltpu.VMEM((BW, BW), BF16),
            pltpu.VMEM((BW, BW), BF16),
            pltpu.VMEM((ACT, GROUPS * BW), F32),
            pltpu.VMEM((GROUPS * BW, BW), BF16),
        ],
        in_specs=[HBM] * 6,
        out_specs=[VMEM] * 6,
        scratch_shapes=[
            pltpu.SMEM((16,), jnp.int32),
            pltpu.SMEM((16,), jnp.int32),
            pltpu.SMEM((2, 16), jnp.int32),
            pltpu.VMEM((ACT, NAO), BF16),
            pltpu.VMEM((NIN, NAO), BF16),
            pltpu.VMEM((BW, PER * BW), F32),
            pltpu.VMEM((SLOTS * BW, GROUPS * BW), BF16),
            pltpu.VMEM((SLOTS, BW, BW), F32),
            pltpu.VMEM((ROWS, 8, BW), F32),
            dma((3,)), dma((SLOTS,)), dma((1,)), dma((SLOTS,)),
        ],
        compiler_params=limit(8192),
        name="contract",
    )(*pinned)
    one, two, three = from_others(message)
    rows = CHIPS * MSG
    keep, send = pl.pallas_call(
        expand_kernel,
        out_shape=[pltpu.VMEM((rows, BW), F32), pltpu.VMEM((rows, BW), BF16)],
        in_specs=[VMEM] * 7,
        out_specs=[VMEM, VMEM],
        scratch_shapes=[
            pltpu.VMEM((ACT, BW), F32),
            pltpu.VMEM((PAIRS, GROUPS * BW), BF16),
            pltpu.VMEM((PAIRS, BW), BF16),
            pltpu.VMEM((SLOTS * BW, BW), F32),
            pltpu.VMEM((PAIRS, BW), F32),
            pltpu.VMEM((PAIRS, BW), F32),
            pltpu.VMEM((rows, BW), F32),
        ],
        compiler_params=limit(8192),
        name="expand",
    )(message, one, two, three, blocks, keep_mask, pick_mask)
    swap = [(0, 1), (1, 0)]
    kept = keep.reshape(NX, NZ * MSG, BW)
    taken = lax.ppermute(send, "core", swap).reshape(NX, NZ * MSG, BW)
    sums = [kept[s] + taken[s].astype(F32) for s in range(NX)]
    one, two, three = from_others([v.astype(BF16) for v in sums], "x")
    pieces = pl.pallas_call(
        along_x_kernel,
        out_shape=pltpu.VMEM((NZ, 80, BW), BF16),
        in_specs=[VMEM] * 4,
        out_specs=VMEM,
        compiler_params=limit(4096),
        name="along_x",
    )(sums[0], one, two, three)
    along_z = lax.all_to_all(pieces, "z", 0, 0, tiled=True)
    pieces = pl.pallas_call(
        route_kernel,
        out_shape=pltpu.VMEM((OWNERS * NX, 48, BW), BF16),
        in_specs=[VMEM] * 2,
        out_specs=VMEM,
        compiler_params=limit(4096),
        name="route",
    )(routes, along_z)
    received = lax.all_to_all(pieces, ("pair", "x"), 0, 0, tiled=True)
    partner = lax.ppermute(received, "core", swap)
    fock, integrals = pl.pallas_call(
        place_kernel,
        out_shape=[
            jax.ShapeDtypeStruct((8 * BW, BW), F32),
            jax.ShapeDtypeStruct((9, PAIRS), F32),
        ],
        in_specs=[VMEM] * 3,
        out_specs=[VMEM, VMEM],
        compiler_params=limit(4096),
        name="place",
    )(places, received, partner)
    return (fock.reshape(8, BW, BW), integrals)


def solution(mesh):
    split = Mesh(mesh.devices.reshape(NX, NZ, CORES, OWNERS), ("x", "z", "core", "pair"))
    aux = ("x", "z", "core")
    return jax.shard_map(
        shards,
        mesh=split,
        in_specs=(P("pair", aux, None, None), P(), P(), P(), P(), P()),
        out_specs=(P("pair", None, None), P(aux, None)),
        check_vma=False,
    )
```
